128 devices in a mesh: batch: 1, cols: 16 (over z, y), rows: 8 (over x, core).
Axes of the slice: x: 4, y: 4, z: 4, core: 2. Of those that a mesh axis runs over, the one named last changes fastest.
Arguments:
- frames: bfloat16 [8, 2, 128, 256, 192], P(None, 'batch', 'rows', 'cols')
- w_x: bfloat16 [3, 3, 192, 768], replicated
- w_h: bfloat16 [3, 3, 192, 768], replicated
- gate_bias: float32 [768], replicated
- h_init: bfloat16 [2, 128, 256, 192], P('batch', 'rows', 'cols')
- c_init: float32 [2, 128, 256, 192], P('batch', 'rows', 'cols')
Outputs:
- output 1: bfloat16 [8, 2, 128, 256, 192], P(None, 'batch', 'rows', 'cols')
- output 2: float32 [2, 128, 256, 192], P('batch', 'rows', 'cols')
All inputs are finite; a program needn't handle non-finite values.
Results may differ from the reference program's by a relative error of at most 0.00162075.
Values are sent between devices in bfloat16 or wider.
A program may use at most 1 GiB of HBM per device.

```python
import jax
import jax.numpy as jnp
from jax import lax

STEPS = 8
SAMPLES = 2
GRID_HEIGHT = 128
GRID_WIDTH = 256
IN_CHANNELS = 192
HIDDEN = 192
BAND_ROWS = 8


def setup_inputs(seed: int = 0, part: int = 0) -> dict:
    root_key = jax.random.key(seed)
    shared_key, local_root = jax.random.split(root_key)
    local_key = jax.random.fold_in(local_root, part)
    key_wx, key_wh, key_bias = jax.random.split(shared_key, 3)
    key_frames, key_hidden, key_cell = jax.random.split(local_key, 3)
    gate_width = 4 * HIDDEN
    frames = jax.random.normal(key_frames, (STEPS, SAMPLES, GRID_HEIGHT, GRID_WIDTH, IN_CHANNELS), jnp.float32)
    w_x = jax.random.normal(key_wx, (3, 3, IN_CHANNELS, gate_width), jnp.float32) * (0.8 * (9 * IN_CHANNELS) ** -0.5)
    w_h = jax.random.normal(key_wh, (3, 3, HIDDEN, gate_width), jnp.float32) * (1.5 * (9 * HIDDEN) ** -0.5)
    forget_shift = jnp.concatenate([jnp.zeros((HIDDEN,), jnp.float32), jnp.ones((HIDDEN,), jnp.float32), jnp.zeros((2 * HIDDEN,), jnp.float32)])
    gate_bias = 0.5 * jax.random.normal(key_bias, (gate_width,), jnp.float32) + forget_shift
    h_init = 0.5 * jax.random.normal(key_hidden, (SAMPLES, GRID_HEIGHT, GRID_WIDTH, HIDDEN), jnp.float32)
    c_init = jax.random.normal(key_cell, (SAMPLES, GRID_HEIGHT, GRID_WIDTH, HIDDEN), jnp.float32)
    return {"frames": frames.astype(jnp.bfloat16), "w_x": w_x.astype(jnp.bfloat16), "w_h": w_h.astype(jnp.bfloat16), "gate_bias": gate_bias, "h_init": h_init.astype(jnp.bfloat16), "c_init": c_init}


def conv_taps(padded, weights, out_rows, out_cols):
    tap_list = [padded[:, row_off:row_off + out_rows, col_off:col_off + out_cols, :] for row_off in range(3) for col_off in range(3)]
    patches = jnp.concatenate(tap_list, axis=-1)
    flat_patches = patches.reshape(-1, patches.shape[-1])
    flat_weights = weights.reshape(-1, weights.shape[-1])
    product = jnp.dot(flat_patches, flat_weights, preferred_element_type=jnp.float32)
    return product.reshape(padded.shape[0], out_rows, out_cols, -1)


def lstm_cell(gate_sum, cell_prev):
    hidden_width = cell_prev.shape[-1]
    in_gate = jax.nn.sigmoid(gate_sum[..., :hidden_width])
    forget_gate = jax.nn.sigmoid(gate_sum[..., hidden_width:2 * hidden_width])
    out_gate = jax.nn.sigmoid(gate_sum[..., 2 * hidden_width:3 * hidden_width])
    cand_gate = jnp.tanh(gate_sum[..., 3 * hidden_width:])
    cell_next = forget_gate * cell_prev + in_gate * cand_gate
    hidden_next = (out_gate * jnp.tanh(cell_next)).astype(jnp.bfloat16)
    return hidden_next, cell_next


def reference(frames, w_x, w_h, gate_bias, h_init, c_init):
    num_bands = GRID_HEIGHT // BAND_ROWS
    pad_cfg = ((0, 0), (1, 1), (1, 1), (0, 0))

    def step_fn(state_pair, frame_t):
        hidden, cell_state = state_pair
        frame_pad = jnp.pad(frame_t, pad_cfg)
        hidden_pad = jnp.pad(hidden, pad_cfg)

        def band_update(band_index):
            row_start = band_index * BAND_ROWS
            frame_band = lax.dynamic_slice_in_dim(frame_pad, row_start, BAND_ROWS + 2, axis=1)
            hidden_band = lax.dynamic_slice_in_dim(hidden_pad, row_start, BAND_ROWS + 2, axis=1)
            cell_band = lax.dynamic_slice_in_dim(cell_state, row_start, BAND_ROWS, axis=1)
            gate_sum = conv_taps(frame_band, w_x, BAND_ROWS, GRID_WIDTH) + conv_taps(hidden_band, w_h, BAND_ROWS, GRID_WIDTH) + gate_bias
            return lstm_cell(gate_sum, cell_band)

        band_hidden, band_cell = lax.map(band_update, jnp.arange(num_bands))
        hidden_next = jnp.moveaxis(band_hidden, 0, 1).reshape(SAMPLES, GRID_HEIGHT, GRID_WIDTH, HIDDEN)
        cell_next = jnp.moveaxis(band_cell, 0, 1).reshape(SAMPLES, GRID_HEIGHT, GRID_WIDTH, HIDDEN)
        return (hidden_next, cell_next), hidden_next

    final_pair, all_hidden = lax.scan(step_fn, (h_init, c_init), frames)
    return all_hidden, final_pair[1]
```

```python
import functools

import jax
import jax.numpy as jnp
from jax import lax
from jax.experimental import pallas as pl
from jax.experimental.pallas import tpu as pltpu
from jax.sharding import PartitionSpec as P

MESH = pl.DeviceIdType.MESH
BF = jnp.bfloat16
F32 = jnp.float32

PITCH = 24
IMG_ROWS = 26
EXT_M = 336
DIRS = ((-1, 0), (1, 0), (0, -1), (0, 1), (-1, -1), (-1, 1), (1, -1), (1, 1))
OPP = (1, 0, 3, 2, 7, 6, 5, 4)


def cell(er, ec):
    return er * PITCH + ec


def corner_src(d):
    return (2 if DIRS[d][0] < 0 else 16), (2 if DIRS[d][1] < 0 else 16)


def corner_dst(d):
    return (18 if DIRS[d][0] < 0 else 0), (18 if DIRS[d][1] < 0 else 0)


def low_lanes(n):
    return lax.broadcasted_iota(jnp.int32, (n, 128), 1) < 64


def twice(v):
    return jnp.concatenate([v, v], axis=1)


def flat(img):
    return img.reshape(2, IMG_ROWS * PITCH, 128)


def put_col(img, er, ec, a, b):
    at = pl.ds(cell(er, ec), 16, stride=PITCH)
    flat(img)[0, at, :] = a
    flat(img)[1, at, :] = b


def get_col(img, lt, er, ec, n=16):
    return flat(img)[lt, pl.ds(cell(er, ec), n, stride=PITCH), :]


def put_rows(img, er, v):
    n = v.shape[0]
    v = v.reshape(n * 16, 192).astype(F32)
    img[0, pl.ds(er, n), 2:18, :] = v[:, :128].reshape(n, 16, 128)
    img[1, pl.ds(er, n), 2:18, :] = twice(v[:, 128:192]).reshape(n, 16, 128)


def build(img, tap, tail, strip, ext):
    first, n = (0, 20) if ext else (1, 18)
    lo = lax.broadcasted_iota(jnp.int32, (n, 16, 128), 2) < 64
    low = lax.broadcasted_iota(jnp.int32, (n - 2, 16, 128), 2) < 64
    for dc in range(3):
        tap[first:first + n, :, dc * 128:(dc + 1) * 128] = img[0, first:first + n, 1 + dc:17 + dc, :].astype(BF)
    b = [img[1, first:first + n, 1 + dc:17 + dc, :] for dc in range(3)]
    tap[first:first + n, :, 384:512] = jnp.where(lo, b[0], b[1]).astype(BF)
    m0, m1 = first * 16, (first + n - 2) * 16
    tail[m0:m1, 0:128] = jnp.where(low, b[2][0:n - 2], b[2][1:n - 1]).astype(BF).reshape(m1 - m0, 128)
    tail[m0:m1, 128:256] = b[2][2:n].astype(BF).reshape(m1 - m0, 128)
    if ext:
        lo24 = low_lanes(24)

        def both(f):
            return jnp.concatenate([f(1), f(18)], axis=0).astype(BF)

        for dr in range(3):
            for dc in range(3):
                strip[dr, :, dc * 128:(dc + 1) * 128] = both(lambda ec: get_col(img, 0, dr, ec + dc - 1, 24))
            strip[dr, :, 384:512] = both(lambda ec: jnp.where(lo24, get_col(img, 1, dr, ec - 1, 24), get_col(img, 1, dr, ec, 24)))
        tail[288:336, 0:128] = both(lambda ec: jnp.where(lo24, get_col(img, 1, 0, ec + 1, 24), get_col(img, 1, 1, ec + 1, 24)))
        tail[288:336, 128:256] = both(lambda ec: get_col(img, 1, 2, ec + 1, 24))


def conv(tap, tail, strip, w, ext):
    if ext:
        blocks = [jnp.concatenate([tap[dr:dr + 18].reshape(288, 512), strip[dr]], axis=0) for dr in range(3)]
        last = tail[:, 0:192]
    else:
        blocks = [tap[1 + dr:17 + dr].reshape(256, 512) for dr in range(3)]
        last = tail[16:272, 0:192]
    lhs = jnp.concatenate(blocks + [last], axis=1)
    return jnp.dot(lhs, w[...], preferred_element_type=F32)


def gates(z, c0, c1):
    n = c0.shape[0]
    lo = low_lanes(n)
    half = jnp.where(lo, 0.5, 1.0).astype(F32)
    off = jnp.where(lo, 0.5, 0.0).astype(F32)
    in0 = 0.5 * jnp.tanh(0.5 * z[0]) + 0.5
    a1 = 0.5 * jnp.tanh(0.5 * z[1]) + 0.5
    a2 = 0.5 * jnp.tanh(0.5 * z[2]) + 0.5
    out0 = 0.5 * jnp.tanh(0.5 * z[3]) + 0.5
    a4 = half * jnp.tanh(half * z[4]) + off
    a5 = jnp.tanh(z[5])
    forget0 = pltpu.roll(jnp.where(lo, a2, a1), 64, 1)
    cand0 = pltpu.roll(jnp.where(lo, a5, a4), 64, 1)
    in_forget1 = jnp.where(lo, a1, a2)
    out_cand1 = jnp.where(lo, a4, a5)
    c0n = forget0 * c0 + in0 * cand0
    prod = in_forget1 * jnp.where(lo, pltpu.roll(out_cand1, 64, 1), c1)
    c1n = prod + pltpu.roll(prod, 64, 1)
    h0 = out0 * jnp.tanh(c0n)
    h1 = out_cand1 * jnp.tanh(c1n)
    h1 = jnp.where(lo, h1, pltpu.roll(h1, 64, 1))
    return h0.astype(BF), h1.astype(BF), c0n, c1n


def kernel(frames, w_x, w_h, bias, h_init, c_init, h_all, c_final,
           fr, hin, cin, wx, wh, imgx, imgh, cst, tapx, tailx, stripx, taph, tailh, striph, gext, gpl, zbuf,
           s_xcol, s_xdiag, r_xrow, r_xcol, r_xdiag,
           s_hcol, s_ccol, s_diag, r_hrow, r_hcol, r_crow, r_ccol, r_diag,
           lsem, wsem, xs_sem, xr_sem, xd_s, xd_r, e_s, e_r, *, shape):
    n_rows, n_cols = shape
    row, col = lax.axis_index("rows"), lax.axis_index("cols")
    grp = lax.axis_index("batch")

    def has(d):
        dr, dc = DIRS[d]
        rr, cc = row + dr, col + dc
        return (rr >= 0) & (rr < n_rows) & (cc >= 0) & (cc < n_cols)

    def peer(d):
        return (grp, col + DIRS[d][1], row + DIRS[d][0])

    loads = [pltpu.make_async_copy(h_init, hin, lsem.at[0]), pltpu.make_async_copy(c_init, cin, lsem.at[1])]
    loads += [pltpu.make_async_copy(frames.at[pl.ds(2 * k, 2)], fr.at[pl.ds(2 * k, 2)], lsem.at[2 + k]) for k in range(4)]
    wloads = [[], []]
    for i, (src, dst) in enumerate(((w_x, wx), (w_h, wh))):
        n = 0
        for dr in range(3):
            for dc in range(3):
                at = dr * 512 + 384 + dc * 64 if dc < 2 else 1536 + dr * 64
                for c_at, rows_n, k_at in ((0, 128, dr * 512 + dc * 128), (128, 64, at)):
                    wloads[i].append(pltpu.make_async_copy(src.at[dr, dc, pl.ds(c_at, rows_n)], dst.at[pl.ds(k_at, rows_n)], wsem.at[i, n]))
                    n += 1
    for cp in loads[2:3] + loads[0:2] + loads[3:4] + wloads[0] + wloads[1] + loads[4:]:
        cp.start()

    barrier = pltpu.get_barrier_semaphore()
    for d in range(8):
        @pl.when(has(d))
        def _(d=d):
            pl.semaphore_signal(barrier, inc=1, device_id=peer(d), device_id_type=MESH)

    for d in range(8):
        @pl.when(jnp.logical_not(has(OPP[d])))
        def _(d=d):
            if d < 2:
                for ref in (r_xrow, r_hrow, r_crow):
                    ref[:, d] = jnp.zeros((ref.shape[0],) + ref.shape[2:], ref.dtype)
            elif d < 4:
                for ref in (r_xcol, r_hcol, r_ccol):
                    ref[:, d - 2] = jnp.zeros((ref.shape[0],) + ref.shape[2:], ref.dtype)
            else:
                for ref in (r_xdiag, r_diag):
                    ref[:, d - 4] = jnp.zeros((ref.shape[0],) + ref.shape[2:], ref.dtype)

    def frame_image(f, s):
        img = imgx.at[2 * f + s]
        put_rows(img, 2, fr[f, s])

    def frame_stage(k, s):
        for odd in range(2):
            f = 2 * k + odd
            img = imgx.at[2 * f + s]
            for side in range(2):
                for j in range(1 if odd else 2):
                    ec = (2 + j) if side == 0 else (17 - j)
                    s_xcol[f, side, j, s, :, 0:128] = get_col(img, 0, 2, ec).astype(BF)
                    s_xcol[f, side, j, s, :, 128:256] = get_col(img, 1, 2, ec).astype(BF)
            for d in range(4, 8):
                er, ec = corner_src(d)
                for lt in range(2):
                    if odd:
                        er1, ec1 = (2 if er == 2 else 17), (2 if ec == 2 else 17)
                        s_xdiag[k, d - 4, s, lt, 4:5, :] = img[lt, er1, pl.ds(ec1, 1), :]
                    else:
                        for i in range(2):
                            s_xdiag[k, d - 4, s, lt, 2 * i:2 * i + 2, :] = img[lt, er + i, pl.ds(ec, 2), :]

    def frame_copy(f, odd, d):
        if d < 2:
            at = (0 if d == 0 else 15) if odd else (0 if d == 0 else 14)
            src = fr.at[f, :, pl.ds(at, 1 if odd else 2)]
            dst = r_xrow.at[f, d, :, pl.ds(d if odd else 0, 1 if odd else 2)]
        else:
            src = s_xcol.at[f, d - 2, pl.ds(0, 1 if odd else 2)]
            dst = r_xcol.at[f, d - 2, pl.ds(0, 1 if odd else 2)]
        return pltpu.make_async_remote_copy(src_ref=src, dst_ref=dst, send_sem=xs_sem.at[f, d], recv_sem=xr_sem.at[f, d], device_id=peer(d), device_id_type=MESH)

    def frame_diag(k, d):
        return pltpu.make_async_remote_copy(src_ref=s_xdiag.at[k, d - 4], dst_ref=r_xdiag.at[k, d - 4], send_sem=xd_s.at[k, d - 4], recv_sem=xd_r.at[k, d - 4], device_id=peer(d), device_id_type=MESH)

    def frame_send(k, odd):
        for d in range(4):
            @pl.when(has(d))
            def _(d=d):
                frame_copy(2 * k + odd, odd, d).start()
        if not odd:
            for d in range(4, 8):
                @pl.when(has(d))
                def _(d=d):
                    frame_diag(k, d).start()

    def frame_wait(k):
        for d in range(8):
            @pl.when(has(OPP[d]))
            def _(d=d):
                if d < 4:
                    frame_copy(2 * k, 0, d).wait_recv()
                    frame_copy(2 * k + 1, 1, d).wait_recv()
                else:
                    frame_diag(k, d).wait_recv()
        for d in range(8):
            @pl.when(has(d))
            def _(d=d):
                if d < 4:
                    frame_copy(2 * k, 0, d).wait_send()
                    frame_copy(2 * k + 1, 1, d).wait_send()
                else:
                    frame_diag(k, d).wait_send()

    def frame_fill(k, odd, s):
        f = 2 * k + odd
        img = imgx.at[2 * f + s]
        for d in range(2):
            i, n = (d, 1) if odd else (0, 2)
            put_rows(img, (18 + i) if d == 0 else i, r_xrow[f, d, s, pl.ds(i, n)])
            for j in range(1 if odd else 2):
                v = r_xcol[f, d, j, s].astype(F32)
                put_col(img, 2, (18 + j) if d == 0 else (1 - j), v[:, 0:128], v[:, 128:256])
        for d in range(4, 8):
            er, ec = corner_dst(d)
            for lt in range(2):
                if odd:
                    er1, ec1 = (18 if er == 18 else 1), (18 if ec == 18 else 1)
                    img[lt, er1, pl.ds(ec1, 1), :] = r_xdiag[k, d - 4, s, lt, 4:5, :]
                else:
                    for i in range(2):
                        img[lt, er + i, pl.ds(ec, 2), :] = r_xdiag[k, d - 4, s, lt, 2 * i:2 * i + 2, :]

    def x_part(k, odd, s):
        img = imgx.at[2 * (2 * k + odd) + s]
        build(img, tapx.at[odd], tailx.at[odd], stripx, not odd)
        z = conv(tapx.at[odd], tailx.at[odd], stripx, wx, not odd)
        if odd:
            gpl[s] = z + bias[...]
        else:
            gext[s] = z + bias[...]

    def state_copies(e, s, d, hsrc):
        x = 2 * e + s

        def mk(src, dst, n):
            return pltpu.make_async_remote_copy(src_ref=src, dst_ref=dst, send_sem=e_s.at[x, n], recv_sem=e_r.at[x, n], device_id=peer(d), device_id_type=MESH)

        if d < 2:
            return [mk(hsrc.at[pl.ds(0 if d == 0 else 14, 2)], r_hrow.at[x, d], d),
                    mk(cst.at[s, :, pl.ds(16 if d == 0 else 256, 16)], r_crow.at[x, d], 8 + d)]
        if d < 4:
            return [mk(s_hcol.at[s, d - 2], r_hcol.at[x, d - 2], d), mk(s_ccol.at[s, d - 2], r_ccol.at[x, d - 2], 8 + d)]
        return [mk(s_diag.at[s, d - 4], r_diag.at[x, d - 4], d)]

    def state_stage(s):
        img = imgh.at[s]
        for side in range(2):
            for j in range(2):
                ec = (2 + j) if side == 0 else (17 - j)
                s_hcol[s, side, j, :, 0:128] = get_col(img, 0, 2, ec).astype(BF)
                s_hcol[s, side, j, :, 128:256] = get_col(img, 1, 2, ec).astype(BF)
            for lt in range(2):
                s_ccol[s, side, lt] = cst[s, lt, pl.ds(16 + 15 * side, 16, stride=16), :]
        for d in range(4, 8):
            er, ec = corner_src(d)
            er1, ec1 = (2 if er == 2 else 17), (2 if ec == 2 else 17)
            for lt in range(2):
                for i in range(2):
                    s_diag[s, d - 4, lt, 2 * i:2 * i + 2, :] = img[lt, er + i, pl.ds(ec, 2), :]
                s_diag[s, d - 4, lt, 4:5, :] = cst[s, lt, pl.ds((er1 - 1) * 16 + ec1 - 2, 1), :]

    def state_send(e, s, hsrc):
        for d in (2, 3, 4, 5, 6, 7, 0, 1):
            @pl.when(has(d))
            def _(d=d):
                for cp in state_copies(e, s, d, hsrc):
                    cp.start()

    def state_wait(e, s, hsrc):
        for d in range(8):
            @pl.when(has(OPP[d]))
            def _(d=d):
                for cp in state_copies(e, s, d, hsrc):
                    cp.wait_recv()
        for d in range(8):
            @pl.when(has(d))
            def _(d=d):
                for cp in state_copies(e, s, d, hsrc):
                    cp.wait_send()

    def state_fill(e, s):
        img = imgh.at[s]
        x = 2 * e + s
        for d in range(2):
            put_rows(img, 18 if d == 0 else 0, r_hrow[x, d])
            for lt in range(2):
                m = 272 if d == 0 else 0
                cst[s, lt, m:m + 16, :] = r_crow[x, d, lt]
            for j in range(2):
                v = r_hcol[x, d, j].astype(F32)
                put_col(img, 2, (18 + j) if d == 0 else (1 - j), v[:, 0:128], v[:, 128:256])
            for lt in range(2):
                m = 288 + (24 if d == 0 else 0) + 1
                cst[s, lt, pl.ds(m, 16), :] = r_ccol[x, d, lt]
        for d in range(4, 8):
            er, ec = corner_dst(d)
            m = 288 + (24 if ec == 18 else 0) + (17 if er == 18 else 0)
            for lt in range(2):
                for i in range(2):
                    img[lt, er + i, pl.ds(ec, 2), :] = r_diag[x, d - 4, lt, 2 * i:2 * i + 2, :]
                cst[s, lt, pl.ds(m, 1), :] = r_diag[x, d - 4, lt, 4:5, :]

    def flag(cond, n):
        return jnp.full((n, 128), jnp.where(cond, 1, 0).astype(jnp.int32)) > 0

    def update(s, t, ext, last=False):
        img = imgh.at[s]

        def unit(er, _):
            m = pl.multiple_of((er - 1) * 16, 16)
            zm = m if ext else pl.multiple_of(m - 16, 16)
            z = [zbuf[pl.ds(zm, 16), n * 128:(n + 1) * 128] for n in range(6)]
            h0, h1, c0, c1 = gates(z, cst[s, 0, pl.ds(m, 16), :], cst[s, 1, pl.ds(m, 16), :])
            cst[s, 0, pl.ds(m, 16), :] = c0
            cst[s, 1, pl.ds(m, 16), :] = c1
            f0, f1 = h0.astype(F32), h1.astype(F32)
            if ext:
                ok = flag(((er > 1) | has(0)) & ((er < 18) | has(1)), 16)
                f0, f1 = jnp.where(ok, f0, 0.0), jnp.where(ok, f1, 0.0)
            img[0, er, 2:18, :] = f0
            img[1, er, 2:18, :] = f1
            return 0

        lax.fori_loop(*((1, 19) if ext else (2, 18)), unit, 0)
        h_all[t, s, :, :, 0:128] = img[0, 2:18, 2:18, :].astype(BF)
        h_all[t, s, :, :, 128:192] = img[1, 2:18, 2:18, :].astype(BF)[:, :, 0:64]
        if last:
            c_final[s, :, :, 0:128] = cst[s, 0, 16:272, :].reshape(16, 16, 128)
            c_final[s, :, :, 128:192] = cst[s, 1, 16:272, :].reshape(16, 16, 128)[:, :, 0:64]
        if not ext:
            return
        pos = lax.broadcasted_iota(jnp.int32, (24, 128), 0)
        for side in range(2):
            ok = flag(has(2 + side), 24) & (flag(has(0), 24) | (pos > 0)) & (flag(has(1), 24) | (pos < 17))
            m = 288 + 24 * side
            z = [zbuf[m:m + 24, n * 128:(n + 1) * 128] for n in range(6)]
            h0, h1, c0, c1 = gates(z, cst[s, 0, m:m + 24, :], cst[s, 1, m:m + 24, :])
            f0, f1 = jnp.where(ok, h0.astype(F32), 0.0), jnp.where(ok, h1.astype(F32), 0.0)
            at = pl.ds(cell(1, 1 + 17 * side), 24, stride=PITCH)
            flat(img)[0, at, :] = f0
            flat(img)[1, at, :] = f1

    def h_step(s, t, ext, last=False):
        build(imgh.at[s], taph, tailh, striph, ext)
        z = conv(taph, tailh, striph, wh, ext)
        if ext:
            zbuf[...] = z + gext[s]
        else:
            zbuf[0:256, :] = z + gpl[s]
        update(s, t, ext, last)

    loads[2].wait()

    def first_frames(s, _):
        frame_image(0, s)
        frame_image(1, s)
        frame_stage(0, s)
        return 0

    lax.fori_loop(0, 2, first_frames, 0)
    loads[0].wait()
    loads[1].wait()

    def first_state(s, _):
        put_rows(imgh.at[s], 2, hin[s])
        v = cin[s].reshape(256, 192)
        cst[s, 0, 16:272, :] = v[:, 0:128]
        cst[s, 1, 16:272, :] = twice(v[:, 128:192])
        state_stage(s)
        return 0

    lax.fori_loop(0, 2, first_state, 0)
    near_rows = 1 + has(0).astype(jnp.int32) + has(1).astype(jnp.int32)
    near_cols = 1 + has(2).astype(jnp.int32) + has(3).astype(jnp.int32)
    pl.semaphore_wait(barrier, near_rows * near_cols - 1)
    frame_send(0, 0)
    def first_send(s, _):
        state_send(0, s, hin.at[s])
        return 0

    lax.fori_loop(0, 2, first_send, 0)
    frame_send(0, 1)
    for cp in loads[3:]:
        cp.wait()

    def stage_body(i, _):
        k, s = i // 2, lax.rem(i, 2)
        frame_image(2 * k, s)
        frame_image(2 * k + 1, s)
        frame_stage(k, s)

        @pl.when(s == 1)
        def _():
            frame_send(k, 0)
            frame_send(k, 1)

        return 0

    lax.fori_loop(2, 8, stage_body, 0)
    for cp in wloads[0]:
        cp.wait()
    frame_wait(0)

    def first_x(s, _):
        for odd in range(2):
            frame_fill(0, odd, s)
            x_part(0, odd, s)
        return 0

    lax.fori_loop(0, 2, first_x, 0)
    for cp in wloads[1]:
        cp.wait()

    def half_round(k, s, final):
        state_fill(k, s)
        h_step(s, 2 * k, True)
        if not final:
            x_part(k + 1, 0, s)
        h_step(s, 2 * k + 1, False, final)
        if not final:
            x_part(k + 1, 1, s)

    def body(i, _):
        k, s = i // 2, lax.rem(i, 2)

        @pl.when(s == 0)
        def _():
            frame_wait(k + 1)

        state_wait(k, s, hin.at[s])
        frame_fill(k + 1, 0, s)
        frame_fill(k + 1, 1, s)
        half_round(k, s, False)
        state_stage(s)
        state_send(k + 1, s, h_all.at[2 * k + 1, s])
        return 0

    def last_body(s, _):
        state_wait(3, s, hin.at[s])
        half_round(3, s, True)
        return 0

    lax.fori_loop(0, 6, body, 0)
    lax.fori_loop(0, 2, last_body, 0)


def solution(mesh):
    shape = (mesh.shape["rows"], mesh.shape["cols"])
    frame_spec = P(None, "batch", "rows", "cols", None)
    state_spec = P("batch", "rows", "cols", None)
    any_spec = pl.BlockSpec(memory_space=pl.ANY)
    vmem = pl.BlockSpec(memory_space=pltpu.VMEM)

    def local_run(frames, w_x, w_h, gate_bias, h_init, c_init):
        V = pltpu.VMEM
        D = pltpu.SemaphoreType.DMA
        scratch = [
            V((8, 2, 16, 16, 192), BF), V((2, 16, 16, 192), BF), V((2, 16, 16, 192), F32),
            V((1728, 768), BF), V((1728, 768), BF),
            V((16, 2, IMG_ROWS, PITCH, 128), F32), V((2, 2, IMG_ROWS, PITCH, 128), F32), V((2, 2, EXT_M, 128), F32),
            V((2, 20, 16, 512), BF), V((2, EXT_M, 256), BF), V((3, 48, 512), BF),
            V((20, 16, 512), BF), V((EXT_M, 256), BF), V((3, 48, 512), BF),
            V((2, EXT_M, 768), F32), V((2, 256, 768), F32), V((EXT_M, 768), F32),
            V((8, 2, 2, 2, 16, 256), BF), V((4, 4, 2, 2, 8, 128), F32),
            V((8, 2, 2, 2, 16, 192), BF), V((8, 2, 2, 2, 16, 256), BF), V((4, 4, 2, 2, 8, 128), F32),
            V((2, 2, 2, 16, 256), BF), V((2, 2, 2, 16, 128), F32), V((2, 4, 2, 8, 128), F32),
            V((8, 2, 2, 16, 192), BF), V((8, 2, 2, 16, 256), BF), V((8, 2, 2, 16, 128), F32), V((8, 2, 2, 16, 128), F32), V((8, 4, 2, 8, 128), F32),
            D((6,)), D((2, 18)), D((8, 4)), D((8, 4)), D((4, 4)), D((4, 4)), D((8, 12)), D((8, 12)),
        ]
        return pl.pallas_call(
            functools.partial(kernel, shape=shape),
            out_shape=[jax.ShapeDtypeStruct(frames.shape, BF), jax.ShapeDtypeStruct(c_init.shape, F32)],
            in_specs=[any_spec, any_spec, any_spec, vmem, any_spec, any_spec],
            out_specs=[vmem, vmem],
            scratch_shapes=scratch,
            compiler_params=pltpu.CompilerParams(collective_id=0, has_side_effects=True, vmem_limit_bytes=60 * 1024 * 1024),
            name="convlstm",
        )(frames, w_x, w_h, gate_bias.reshape(1, -1), h_init, c_init)

    return jax.shard_map(local_run, mesh=mesh, in_specs=(frame_spec, P(), P(), P(), state_spec, state_spec), out_specs=(frame_spec, state_spec), check_vma=False)
```

```python
import functools

import jax
import jax.numpy as jnp
from jax import lax
from jax.experimental import pallas as pl
from jax.experimental.pallas import tpu as pltpu
from jax.sharding import PartitionSpec as P

MESH = pl.DeviceIdType.MESH
BF = jnp.bfloat16
F32 = jnp.float32

L, HALF, SIDE, CH, GATES, TAPS = 128, 64, 16, 192, 768, 512
LO, HI = slice(0, L), slice(L, 2 * L)
TWO, FOUR, EIGHT, FAR = 2, 4, 8, 18
PITCH = 24
IMG_ROWS = 26
STRIP = 24
MAIN = 288
EXT_M = 336
PLAIN_M = 256
DIRS = ((-1, 0), (1, 0), (0, -1), (0, 1), (-1, -1), (-1, 1), (1, -1), (1, 1))
OPP = (1, 0, 3, 2, 7, 6, 5, 4)


def cell(er, ec):
    return er * PITCH + ec


def corner_src(d):
    return (TWO if DIRS[d][0] < 0 else 16), (TWO if DIRS[d][1] < 0 else 16)


def corner_dst(d):
    return (FAR if DIRS[d][0] < 0 else 0), (FAR if DIRS[d][1] < 0 else 0)


def low_lanes(n):
    return lax.broadcasted_iota(jnp.int32, (n, 128), 1) < 64


def twice(v):
    return jnp.concatenate([v, v], axis=1)


def flat(img):
    return img.reshape(TWO, IMG_ROWS * PITCH, L)


def put_col(img, er, ec, a, b, n=SIDE):
    at = pl.ds(cell(er, ec), n, stride=PITCH)
    flat(img)[0, at, :] = a
    flat(img)[1, at, :] = b


def get_col(img, lt, er, ec, n=SIDE):
    return flat(img)[lt, pl.ds(cell(er, ec), n, stride=PITCH), :]


def put_rows(img, er, v):
    n = v.shape[0]
    v = v.reshape(n * SIDE, CH).astype(F32)
    put_body(img, er, v[:, LO], twice(v[:, L:CH]))


def put_body(img, er, a, b):
    n = a.shape[0] // SIDE
    for lt, v in enumerate((a, b)):
        img[lt, pl.ds(er, n), TWO:TWO + SIDE, :] = v.reshape(n, SIDE, L)


def build(img, lhs, ext):
    tap, tail, strip = lhs
    first, n = (0, 20) if ext else (1, FAR)
    rows = slice(first, first + n)
    lo = lax.broadcasted_iota(jnp.int32, (n, SIDE, L), TWO) < HALF
    for dc in range(3):
        tap[rows, :, dc * L:(dc + 1) * L] = img[0, rows, 1 + dc:17 + dc, :].astype(BF)
    b = [img[1, rows, 1 + dc:17 + dc, :] for dc in range(3)]
    tap[rows, :, 3 * L:TAPS] = jnp.where(lo, b[0], b[1]).astype(BF)
    m = n - TWO
    at = pl.ds(first * SIDE, m * SIDE)
    tail[at, LO] = jnp.where(lo[:m], b[TWO][:m], b[TWO][1:n - 1]).astype(BF).reshape(m * SIDE, L)
    tail[at, HI] = b[TWO][TWO:n].astype(BF).reshape(m * SIDE, L)
    if ext:
        lo24 = low_lanes(STRIP)

        def both(f):
            return jnp.concatenate([f(1), f(FAR)], axis=0).astype(BF)

        def col(lt, er, ec):
            return get_col(img, lt, er, ec, STRIP)

        for dr in range(3):
            for dc in range(3):
                strip[dr, :, dc * L:(dc + 1) * L] = both(lambda ec: col(0, dr, ec + dc - 1))
            strip[dr, :, 3 * L:TAPS] = both(lambda ec: jnp.where(lo24, col(1, dr, ec - 1), col(1, dr, ec)))
        tail[MAIN:EXT_M, LO] = both(lambda ec: jnp.where(lo24, col(1, 0, ec + 1), col(1, 1, ec + 1)))
        tail[MAIN:EXT_M, HI] = both(lambda ec: col(1, TWO, ec + 1))


def operand(lhs, ext):
    tap, tail, strip = lhs
    if ext:
        blocks = [jnp.concatenate([tap[dr:dr + FAR].reshape(MAIN, TAPS), strip[dr]], axis=0) for dr in range(3)]
        last = tail[:, 0:CH]
    else:
        blocks = [tap[1 + dr:17 + dr].reshape(PLAIN_M, TAPS) for dr in range(3)]
        last = tail[SIDE:SIDE + PLAIN_M, 0:CH]
    return jnp.concatenate(blocks + [last], axis=1)


def conv(lhs, w, add, out, ext, parts):
    x = operand(lhs, ext)
    for p in parts:
        at = slice(p * TWO * L, (p + 1) * TWO * L)
        z = jnp.dot(x, w[:, at], preferred_element_type=F32)
        out[:, at] = z + (add[:, at] if len(add.shape) > 1 else add[at].reshape(1, TWO * L))


def gates(z, c0, c1):
    n = c0.shape[0]
    lo = low_lanes(n)
    half = jnp.where(lo, 0.5, 1.0).astype(F32)
    off = jnp.where(lo, 0.5, 0.0).astype(F32)
    in0 = 0.5 * jnp.tanh(0.5 * z[0]) + 0.5
    a1 = 0.5 * jnp.tanh(0.5 * z[1]) + 0.5
    a2 = 0.5 * jnp.tanh(0.5 * z[TWO]) + 0.5
    out0 = 0.5 * jnp.tanh(0.5 * z[3]) + 0.5
    a4 = half * jnp.tanh(half * z[FOUR]) + off
    a5 = jnp.tanh(z[5])
    forget0 = pltpu.roll(jnp.where(lo, a2, a1), 64, 1)
    cand0 = pltpu.roll(jnp.where(lo, a5, a4), 64, 1)
    in_forget1 = jnp.where(lo, a1, a2)
    out_cand1 = jnp.where(lo, a4, a5)
    c0n = forget0 * c0 + in0 * cand0
    prod = in_forget1 * jnp.where(lo, pltpu.roll(out_cand1, 64, 1), c1)
    c1n = prod + pltpu.roll(prod, 64, 1)
    h0 = out0 * jnp.tanh(c0n)
    h1 = out_cand1 * jnp.tanh(c1n)
    h1 = jnp.where(lo, h1, pltpu.roll(h1, 64, 1))
    return h0.astype(BF), h1.astype(BF), c0n, c1n


def kernel(frames, w_x, w_h, bias, h_init, c_init, h_all, c_final,
           fr, hin, cin, wx, wh, imgx, imgh, cst, tapx, tailx, stripx, tapy, taily, taph, tailh, striph, gext, gpl, zext, zpl,
           s_xcol, s_xdiag, r_xrow, r_xcol, r_xdiag,
           s_hcol, s_ccol, s_diag, r_hrow, r_hcol, r_crow, r_ccol, r_diag,
           lsem, wsem, xs_sem, xr_sem, xd_s, xd_r, e_s, e_r, *, shape):
    lhs_x, lhs_y, lhs_h = (tapx, tailx, stripx), (tapy, taily, None), (taph, tailh, striph)
    n_rows, n_cols = shape
    row, col = lax.axis_index("rows"), lax.axis_index("cols")
    grp = lax.axis_index("batch")

    def has(d):
        dr, dc = DIRS[d]
        rr, cc = row + dr, col + dc
        return (rr >= 0) & (rr < n_rows) & (cc >= 0) & (cc < n_cols)

    def peer(d):
        return (grp, col + DIRS[d][1], row + DIRS[d][0])

    loads = [pltpu.make_async_copy(h_init, hin, lsem.at[0]), pltpu.make_async_copy(c_init, cin, lsem.at[1])]
    loads += [pltpu.make_async_copy(frames.at[pl.ds(TWO * k, TWO)], fr.at[pl.ds(TWO * k, TWO)], lsem.at[TWO + k]) for k in range(FOUR)]
    wloads = [[], []]
    for i, (src, dst) in enumerate(((w_x, wx), (w_h, wh))):
        n = 0
        for dr in range(3):
            for dc in range(3):
                at = dr * 512 + 384 + dc * 64 if dc < TWO else 1536 + dr * 64
                for c_at, rows_n, k_at in ((0, 128, dr * 512 + dc * 128), (128, 64, at)):
                    wloads[i].append(pltpu.make_async_copy(src.at[dr, dc, pl.ds(c_at, rows_n)], dst.at[pl.ds(k_at, rows_n)], wsem.at[i, n]))
                    n += 1
    for cp in loads[TWO:3] + loads[0:TWO] + loads[3:FOUR] + wloads[0] + wloads[1] + loads[FOUR:]:
        cp.start()

    barrier = pltpu.get_barrier_semaphore()
    for d in range(EIGHT):
        @pl.when(has(d))
        def _(d=d):
            pl.semaphore_signal(barrier, inc=1, device_id=peer(d), device_id_type=MESH)

    for d in range(EIGHT):
        @pl.when(jnp.logical_not(has(OPP[d])))
        def _(d=d):
            if d < TWO:
                for ref in (r_xrow, r_hrow, r_crow):
                    ref[:, d] = jnp.zeros((ref.shape[0],) + ref.shape[TWO:], ref.dtype)
            elif d < FOUR:
                for ref in (r_xcol, r_hcol, r_ccol):
                    ref[:, d - TWO] = jnp.zeros((ref.shape[0],) + ref.shape[TWO:], ref.dtype)
            else:
                for ref in (r_xdiag, r_diag):
                    ref[:, d - FOUR] = jnp.zeros((ref.shape[0],) + ref.shape[TWO:], ref.dtype)

    def frame_image(f, s):
        put_rows(imgx.at[TWO * f + s], TWO, fr[f, s])

    def frame_stage(k, s):
        for odd in range(TWO):
            f = TWO * k + odd
            img = imgx.at[TWO * f + s]
            for side in range(TWO):
                for j in range(1 if odd else TWO):
                    ec = (TWO + j) if side == 0 else (17 - j)
                    for lt, at in enumerate((LO, HI)):
                        s_xcol[f, side, j, s, :, at] = get_col(img, lt, TWO, ec).astype(BF)
            for d in range(FOUR, EIGHT):
                er, ec = corner_src(d)
                for lt in range(TWO):
                    if odd:
                        er1, ec1 = (TWO if er == TWO else 17), (TWO if ec == TWO else 17)
                        s_xdiag[k, d - FOUR, s, lt, FOUR:5, :] = img[lt, er1, pl.ds(ec1, 1), :]
                    else:
                        for i in range(TWO):
                            s_xdiag[k, d - FOUR, s, lt, TWO * i:TWO * i + TWO, :] = img[lt, er + i, pl.ds(ec, TWO), :]

    def frame_copy(f, odd, d):
        if d < TWO:
            at = (0 if d == 0 else 15) if odd else (0 if d == 0 else 14)
            src = fr.at[f, :, pl.ds(at, 1 if odd else TWO)]
            dst = r_xrow.at[f, d, :, pl.ds(d if odd else 0, 1 if odd else TWO)]
        else:
            src = s_xcol.at[f, d - TWO, pl.ds(0, 1 if odd else TWO)]
            dst = r_xcol.at[f, d - TWO, pl.ds(0, 1 if odd else TWO)]
        return pltpu.make_async_remote_copy(src_ref=src, dst_ref=dst, send_sem=xs_sem.at[f, d], recv_sem=xr_sem.at[f, d], device_id=peer(d), device_id_type=MESH)

    def frame_diag(k, d):
        return pltpu.make_async_remote_copy(src_ref=s_xdiag.at[k, d - FOUR], dst_ref=r_xdiag.at[k, d - FOUR], send_sem=xd_s.at[k, d - FOUR], recv_sem=xd_r.at[k, d - FOUR], device_id=peer(d), device_id_type=MESH)

    def frame_send(k, odd):
        for d in range(FOUR):
            @pl.when(has(d))
            def _(d=d):
                frame_copy(TWO * k + odd, odd, d).start()
        if not odd:
            for d in range(FOUR, EIGHT):
                @pl.when(has(d))
                def _(d=d):
                    frame_diag(k, d).start()

    def frame_wait(k):
        for d in range(EIGHT):
            @pl.when(has(OPP[d]))
            def _(d=d):
                if d < FOUR:
                    frame_copy(TWO * k, 0, d).wait_recv()
                    frame_copy(TWO * k + 1, 1, d).wait_recv()
                else:
                    frame_diag(k, d).wait_recv()
        for d in range(EIGHT):
            @pl.when(has(d))
            def _(d=d):
                if d < FOUR:
                    frame_copy(TWO * k, 0, d).wait_send()
                    frame_copy(TWO * k + 1, 1, d).wait_send()
                else:
                    frame_diag(k, d).wait_send()

    def frame_fill(k, odd, s):
        f = TWO * k + odd
        img = imgx.at[TWO * f + s]
        for d in range(TWO):
            i, n = (d, 1) if odd else (0, TWO)
            put_rows(img, (FAR + i) if d == 0 else i, r_xrow[f, d, s, pl.ds(i, n)])
            for j in range(1 if odd else TWO):
                v = r_xcol[f, d, j, s].astype(F32)
                put_col(img, TWO, (FAR + j) if d == 0 else (1 - j), v[:, LO], v[:, HI])
        for d in range(FOUR, EIGHT):
            er, ec = corner_dst(d)
            for lt in range(TWO):
                if odd:
                    er1, ec1 = (FAR if er == FAR else 1), (FAR if ec == FAR else 1)
                    img[lt, er1, pl.ds(ec1, 1), :] = r_xdiag[k, d - FOUR, s, lt, FOUR:5, :]
                else:
                    for i in range(TWO):
                        img[lt, er + i, pl.ds(ec, TWO), :] = r_xdiag[k, d - FOUR, s, lt, TWO * i:TWO * i + TWO, :]

    def x_build(k, odd, s):
        frame_fill(k, odd, s)
        build(imgx.at[TWO * (TWO * k + odd) + s], lhs_y if odd else lhs_x, not odd)

    def x_conv(s, odd, parts):
        if odd:
            conv(lhs_y, wx, bias, gpl.at[s], False, parts)
        else:
            conv(lhs_x, wx, bias, gext.at[s], True, parts)

    def state_copies(e, s, d, hsrc):
        x = TWO * e + s

        def mk(src, dst, n):
            return pltpu.make_async_remote_copy(src_ref=src, dst_ref=dst, send_sem=e_s.at[x, n], recv_sem=e_r.at[x, n], device_id=peer(d), device_id_type=MESH)

        if d < TWO:
            return [mk(hsrc.at[pl.ds(0 if d == 0 else 14, TWO)], r_hrow.at[x, d], d),
                    mk(cst.at[s, :, pl.ds(16 if d == 0 else 256, 16)], r_crow.at[x, d], EIGHT + d)]
        if d < FOUR:
            return [mk(s_hcol.at[s, d - TWO], r_hcol.at[x, d - TWO], d), mk(s_ccol.at[s, d - TWO], r_ccol.at[x, d - TWO], EIGHT + d)]
        return [mk(s_diag.at[s, d - FOUR], r_diag.at[x, d - FOUR], d)]

    def state_stage(s):
        img = imgh.at[s]
        for side in range(TWO):
            for j in range(TWO):
                ec = (TWO + j) if side == 0 else (17 - j)
                for lt, at in enumerate((LO, HI)):
                    s_hcol[s, side, j, :, at] = get_col(img, lt, TWO, ec).astype(BF)
            for lt in range(TWO):
                s_ccol[s, side, lt] = cst[s, lt, pl.ds(16 + 15 * side, 16, stride=16), :]
        for d in range(FOUR, EIGHT):
            er, ec = corner_src(d)
            er1, ec1 = (TWO if er == TWO else 17), (TWO if ec == TWO else 17)
            for lt in range(TWO):
                for i in range(TWO):
                    s_diag[s, d - FOUR, lt, TWO * i:TWO * i + TWO, :] = img[lt, er + i, pl.ds(ec, TWO), :]
                s_diag[s, d - FOUR, lt, FOUR:5, :] = cst[s, lt, pl.ds((er1 - 1) * 16 + ec1 - TWO, 1), :]

    def state_send(e, s, hsrc):
        for d in (TWO, 3, FOUR, 5, 6, 7, 0, 1):
            @pl.when(has(d))
            def _(d=d):
                for cp in state_copies(e, s, d, hsrc):
                    cp.start()

    def state_wait(e, s):
        for d in range(EIGHT):
            @pl.when(has(OPP[d]))
            def _(d=d):
                for cp in state_copies(e, s, d, hin.at[s]):
                    cp.wait_recv()
        for d in range(EIGHT):
            @pl.when(has(d))
            def _(d=d):
                for cp in state_copies(e, s, d, hin.at[s]):
                    cp.wait_send()

    def state_fill(e, s):
        img = imgh.at[s]
        x = TWO * e + s
        for d in range(TWO):
            put_rows(img, FAR if d == 0 else 0, r_hrow[x, d])
            for lt in range(TWO):
                m = 272 if d == 0 else 0
                cst[s, lt, m:m + 16, :] = r_crow[x, d, lt]
            for j in range(TWO):
                v = r_hcol[x, d, j].astype(F32)
                put_col(img, TWO, (FAR + j) if d == 0 else (1 - j), v[:, LO], v[:, HI])
            for lt in range(TWO):
                m = 288 + (24 if d == 0 else 0) + 1
                cst[s, lt, pl.ds(m, 16), :] = r_ccol[x, d, lt]
        for d in range(FOUR, EIGHT):
            er, ec = corner_dst(d)
            m = 288 + (24 if ec == FAR else 0) + (17 if er == FAR else 0)
            for lt in range(TWO):
                for i in range(TWO):
                    img[lt, er + i, pl.ds(ec, TWO), :] = r_diag[x, d - FOUR, lt, TWO * i:TWO * i + TWO, :]
                cst[s, lt, pl.ds(m, 1), :] = r_diag[x, d - FOUR, lt, FOUR:5, :]

    def flag(cond, n):
        return jnp.full((n, 128), jnp.where(cond, 1, 0).astype(jnp.int32)) > 0

    def update(s, t, ext, last=False):
        img = imgh.at[s]
        z_ref = zext if ext else zpl

        def one(m, n):
            zm = m if ext else m - SIDE
            z = [z_ref[zm:zm + n, p * L:(p + 1) * L] for p in range(6)]
            h0, h1, c0, c1 = gates(z, cst[s, 0, m:m + n, :], cst[s, 1, m:m + n, :])
            cst[s, 0, m:m + n, :] = c0
            cst[s, 1, m:m + n, :] = c1
            return h0, h1, c0, c1

        er, end = (1, 19) if ext else (TWO, FAR)
        while er < end:
            n = 1 if er == 1 or er == end - 1 else TWO
            h0, h1, c0, c1 = one((er - 1) * SIDE, n * SIDE)
            if 1 < er < FAR:
                at = pl.ds(er - TWO, n)
                h_all[t, s, at, :, LO] = h0.reshape(n, SIDE, L)
                h_all[t, s, at, :, L:CH] = h1[:, :HALF].reshape(n, SIDE, HALF)
            if last:
                c_final[s, at, :, LO] = c0.reshape(n, SIDE, L)
                c_final[s, at, :, L:CH] = c1[:, :HALF].reshape(n, SIDE, HALF)
            else:
                f0, f1 = h0.astype(F32), h1.astype(F32)
                if er == 1 or er == FAR:
                    ok = flag(has(0 if er == 1 else 1), n * SIDE)
                    f0, f1 = jnp.where(ok, f0, 0.0), jnp.where(ok, f1, 0.0)
                put_body(img, er, f0, f1)
            er += n
        if not ext:
            return
        pos = lax.broadcasted_iota(jnp.int32, (STRIP, L), 0)
        for side in range(TWO):
            ok = flag(has(TWO + side), STRIP) & (flag(has(0), STRIP) | (pos > 0)) & (flag(has(1), STRIP) | (pos < 17))
            h0, h1, _, _ = one(MAIN + STRIP * side, STRIP)
            put_col(img, 1, 1 + 17 * side, jnp.where(ok, h0.astype(F32), 0.0), jnp.where(ok, h1.astype(F32), 0.0), STRIP)

    def h_build(s, ext):
        build(imgh.at[s], lhs_h, ext)

    def h_conv(s, ext):
        if ext:
            conv(lhs_h, wh, gext.at[s], zext, True, range(3))
        else:
            conv(lhs_h, wh, gpl.at[s], zpl, False, range(3))

    loads[TWO].wait()

    def first_frames(s, _):
        frame_image(0, s)
        frame_image(1, s)
        frame_stage(0, s)
        return 0

    lax.fori_loop(0, TWO, first_frames, 0)
    loads[0].wait()
    loads[1].wait()

    def first_state(s, _):
        put_rows(imgh.at[s], TWO, hin[s])
        v = cin[s].reshape(256, 192)
        cst[s, 0, 16:272, :] = v[:, 0:128]
        cst[s, 1, 16:272, :] = twice(v[:, 128:192])
        state_stage(s)
        return 0

    lax.fori_loop(0, TWO, first_state, 0)
    near_rows = 1 + has(0).astype(jnp.int32) + has(1).astype(jnp.int32)
    near_cols = 1 + has(TWO).astype(jnp.int32) + has(3).astype(jnp.int32)
    pl.semaphore_wait(barrier, near_rows * near_cols - 1)
    frame_send(0, 0)
    def first_send(s, _):
        state_send(0, s, hin.at[s])
        return 0

    lax.fori_loop(0, TWO, first_send, 0)
    frame_send(0, 1)
    for cp in loads[3:]:
        cp.wait()

    def stage_body(i, _):
        k, s = i // TWO, lax.rem(i, TWO)
        frame_image(TWO * k, s)
        frame_image(TWO * k + 1, s)
        frame_stage(k, s)

        @pl.when(s == 1)
        def _():
            frame_send(k, 0)
            frame_send(k, 1)

        return 0

    lax.fori_loop(TWO, EIGHT, stage_body, 0)
    for cp in wloads[0]:
        cp.wait()
    frame_wait(0)

    for s in range(TWO):
        x_build(0, 0, s)
        x_conv(s, 0, range(3))
        x_build(0, 1, s)
        x_conv(s, 1, range(3) if s == 0 else range(TWO))
    for cp in wloads[1]:
        cp.wait()

    def half_round(k, s):
        x_conv(1 - s, 1, (TWO,))
        state_fill(k, s)
        h_build(s, True)
        x_build(k + 1, 0, s)
        h_conv(s, True)
        x_conv(s, 0, (0, 1))
        update(s, TWO * k, True)
        h_build(s, False)
        x_build(k + 1, 1, s)
        h_conv(s, False)
        x_conv(s, 0, (TWO,))
        x_conv(s, 1, (0,))
        update(s, TWO * k + 1, False)
        state_stage(s)

    def round_body(k, _):
        frame_wait(k + 1)
        for s in range(TWO):
            state_wait(k, s)
            half_round(k, s)
            state_send(k + 1, s, h_all.at[TWO * k + 1, s])
            x_conv(s, 1, (1,))
        return 0

    lax.fori_loop(0, 3, round_body, 0)
    last = 3
    state_wait(last, 0)
    x_conv(1, 1, (TWO,))
    state_fill(last, 0)
    h_build(0, True)
    h_conv(0, True)
    update(0, TWO * last, True)
    state_wait(last, 1)
    state_fill(last, 1)
    h_build(1, True)
    h_conv(1, True)
    h_build(0, False)
    h_conv(0, False)
    update(1, TWO * last, True)
    h_build(1, False)
    update(0, TWO * last + 1, False, True)
    h_conv(1, False)
    update(1, TWO * last + 1, False, True)


def solution(mesh):
    shape = (mesh.shape["rows"], mesh.shape["cols"])
    frame_spec = P(None, "batch", "rows", "cols", None)
    state_spec = P("batch", "rows", "cols", None)
    any_spec = pl.BlockSpec(memory_space=pl.ANY)
    vmem = pl.BlockSpec(memory_space=pltpu.VMEM)

    def local_run(frames, w_x, w_h, gate_bias, h_init, c_init):
        V = pltpu.VMEM
        D = pltpu.SemaphoreType.DMA
        scratch = [
            V(frames.shape, BF), V(h_init.shape, BF), V(c_init.shape, F32),
            V((9 * CH, GATES), BF), V((9 * CH, GATES), BF),
            V((16, TWO, IMG_ROWS, PITCH, L), F32), V((TWO, TWO, IMG_ROWS, PITCH, L), F32), V((TWO, TWO, EXT_M, L), F32),
            V((20, SIDE, TAPS), BF), V((EXT_M, TWO * L), BF), V((3, TWO * STRIP, TAPS), BF),
            V((20, SIDE, TAPS), BF), V((EXT_M, TWO * L), BF),
            V((20, SIDE, TAPS), BF), V((EXT_M, TWO * L), BF), V((3, TWO * STRIP, TAPS), BF),
            V((TWO, EXT_M, GATES), F32), V((TWO, PLAIN_M, GATES), F32), V((EXT_M, GATES), F32), V((PLAIN_M, GATES), F32),
            V((EIGHT, TWO, TWO, TWO, SIDE, TWO * L), BF), V((FOUR, FOUR, TWO, TWO, EIGHT, L), F32),
            V((EIGHT, TWO, TWO, TWO, SIDE, CH), BF), V((EIGHT, TWO, TWO, TWO, SIDE, TWO * L), BF), V((FOUR, FOUR, TWO, TWO, EIGHT, L), F32),
            V((TWO, TWO, TWO, SIDE, TWO * L), BF), V((TWO, TWO, TWO, SIDE, L), F32), V((TWO, FOUR, TWO, EIGHT, L), F32),
            V((EIGHT, TWO, TWO, SIDE, CH), BF), V((EIGHT, TWO, TWO, SIDE, TWO * L), BF), V((EIGHT, TWO, TWO, SIDE, L), F32), V((EIGHT, TWO, TWO, SIDE, L), F32), V((EIGHT, FOUR, TWO, EIGHT, L), F32),
            D((6,)), D((TWO, FAR)), D((EIGHT, FOUR)), D((EIGHT, FOUR)), D((FOUR, FOUR)), D((FOUR, FOUR)), D((EIGHT, 12)), D((EIGHT, 12)),
        ]
        return pl.pallas_call(
            functools.partial(kernel, shape=shape),
            out_shape=[V(frames.shape, BF), V(c_init.shape, F32)],
            in_specs=[any_spec, any_spec, any_spec, vmem, any_spec, any_spec],
            out_specs=[vmem, vmem],
            scratch_shapes=scratch,
            compiler_params=pltpu.CompilerParams(collective_id=0, has_side_effects=True, vmem_limit_bytes=60 * 1024 * 1024),
            name="convlstm",
        )(frames, w_x, w_h, gate_bias, h_init, c_init)

    return jax.shard_map(local_run, mesh=mesh, in_specs=(frame_spec, P(), P(), P(), state_spec, state_spec), out_specs=(frame_spec, state_spec), check_vma=False)
```

```python
import functools

import jax
import jax.numpy as jnp
from jax import lax
from jax.experimental import pallas as pl
from jax.experimental.pallas import tpu as pltpu
from jax.sharding import PartitionSpec as P

MESH = pl.DeviceIdType.MESH
BF = jnp.bfloat16
F32 = jnp.float32

L, HALF, SIDE, CH, GATES, TAPS = 128, 64, 16, 192, 768, 512
TWO, FOUR, EIGHT, FAR = 2, 4, 8, 18
PIECES = 6
PITCH = 24
IMG_ROWS = 26
STRIP = 24
MAIN = 288
EXT_M = 336
PLAIN_M = 256
INNER = 14
DIRS = ((-1, 0), (1, 0), (0, -1), (0, 1), (-1, -1), (-1, 1), (1, -1), (1, 1))
OPP = (1, 0, 3, 2, 7, 6, 5, 4)
STRIPS = ((1, 1, STRIP), (FAR, 1, STRIP), (2, 3, SIDE), (17, 3, SIDE))
STRIP_M = 80
EXT = (((1, FAR),), slice(0, 48))
PLAIN = (((2, SIDE),), None)
IN = (((3, INNER),), None)
EXT_OUT = (((1, 2), (17, 2)), slice(0, STRIP_M))
PLAIN_OUT = (((2, 1), (17, 1)), slice(48, STRIP_M))


def cell(er, ec):
    return er * PITCH + ec


def corner_src(d):
    return (TWO if DIRS[d][0] < 0 else SIDE), (TWO if DIRS[d][1] < 0 else SIDE)


def corner_dst(d):
    return (FAR if DIRS[d][0] < 0 else 0), (FAR if DIRS[d][1] < 0 else 0)


def near(e):
    return {TWO: TWO, SIDE: 17, FAR: FAR, 0: 1}[e]


def low_lanes(n):
    return lax.broadcasted_iota(jnp.int32, (n, L), 1) < HALF


def twice(v):
    return jnp.concatenate([v, v], axis=1)


def halves(v):
    lo, w = low_lanes(v.shape[0]), pltpu.roll(v, HALF, 1)
    return jnp.where(lo, v, w), jnp.where(lo, w, v)


def join(a, b):
    return jnp.where(low_lanes(a.shape[0]), a, b)


def flat(ref):
    return ref.reshape(ref.shape[0], TWO, IMG_ROWS * PITCH, L)


def put_col(img, er, ec, a, b):
    ref, x = img
    at = pl.ds(cell(er, ec), a.shape[0], stride=PITCH)
    flat(ref)[x, 0, at, :] = a
    flat(ref)[x, 1, at, :] = b


def get_col(img, lt, er, ec, n=SIDE):
    ref, x = img
    return flat(ref)[x, lt, pl.ds(cell(er, ec), n, stride=PITCH), :]


def put_rows(img, er, v):
    n = v.shape[0]
    v = v.reshape(n * SIDE, CH).astype(F32)
    put_body(img, er, v[:, :L], twice(v[:, L:]))


def put_body(img, er, a, b):
    n = a.shape[0] // SIDE
    ref, x = img
    for lt, v in enumerate((a, b)):
        ref[x, lt, pl.ds(er, n), TWO:FAR, :] = v.reshape(n, SIDE, L)


def pack_cols(dst, a0, b0, a1, b1):
    for i, v in enumerate((a0, a1, join(b0, b1))):
        dst[i] = v.astype(dst.dtype)


def unpack_cols(src):
    b0, b1 = halves(src[TWO].astype(F32))
    return src[0].astype(F32), b0, src[1].astype(F32), b1


def pack_corner(dst, img, d, a, b):
    er, ec = corner_src(d)
    ref, x = img
    for i in range(TWO):
        dst[TWO * i:TWO * i + TWO, :] = ref[x, 0, er + i, pl.ds(ec, TWO), :]
        dst[5 + i:6 + i, :] = join(ref[x, 1, er + i, pl.ds(ec, 1), :], ref[x, 1, er + i, pl.ds(ec + 1, 1), :])
    dst[FOUR:5, :] = a
    dst[7:EIGHT, :] = b


def unpack_corner(src, img, d):
    er, ec = corner_dst(d)
    ref, x = img
    for i in range(TWO):
        ref[x, 0, er + i, pl.ds(ec, TWO), :] = src[TWO * i:TWO * i + TWO, :]
        for j, v in enumerate(halves(src[5 + i:6 + i, :])):
            ref[x, 1, er + i, pl.ds(ec + j, 1), :] = v


def build_rows(img, lhs, first, n):
    tap, tail, _ = lhs
    ref, x = img
    rows = slice(first, first + n)
    lo = lax.broadcasted_iota(jnp.int32, (n, SIDE, L), TWO) < HALF
    for dc in range(3):
        tap[rows, :, dc * L:(dc + 1) * L] = ref[x, 0, rows, 1 + dc:17 + dc, :].astype(BF)
    b = [ref[x, 1, rows, 1 + dc:17 + dc, :] for dc in range(3)]
    tap[rows, :, 3 * L:] = jnp.where(lo, b[0], b[1]).astype(BF)
    m = n - TWO
    at = pl.ds(first * SIDE, m * SIDE)
    tail[at, :L] = jnp.where(lo[:m], b[TWO][:m], b[TWO][1:n - 1]).astype(BF).reshape(m * SIDE, L)
    tail[at, L:] = b[TWO][TWO:].astype(BF).reshape(m * SIDE, L)


def build_strips(img, lhs, which):
    _, tail, strip = lhs
    at = 0
    for ec, er, n in STRIPS:
        rows = slice(at, at + n)
        at += n
        if (ec, er, n) not in which:
            continue

        def col(lt, dr, dc):
            return get_col(img, lt, er - 1 + dr, ec - 1 + dc, n)

        for dr in range(3):
            for dc in range(3):
                strip[dr, rows, dc * L:(dc + 1) * L] = col(0, dr, dc).astype(BF)
            strip[dr, rows, 3 * L:] = join(col(1, dr, 0), col(1, dr, 1)).astype(BF)
        rows = slice(MAIN + rows.start, MAIN + rows.stop)
        tail[rows, :L] = join(col(1, 0, TWO), col(1, 1, TWO)).astype(BF)
        tail[rows, L:] = col(1, TWO, TWO).astype(BF)


def build(img, lhs, kind):
    if kind is EXT:
        build_rows(img, lhs, 0, 20)
        build_strips(img, lhs, STRIPS[:TWO])
    elif kind is PLAIN:
        build_rows(img, lhs, 1, FAR)
    elif kind is IN:
        build_rows(img, lhs, TWO, SIDE)
    elif kind is EXT_OUT:
        build_rows(img, lhs, 0, FOUR)
        build_rows(img, lhs, SIDE, FOUR)
        build_strips(img, lhs, STRIPS)
    else:
        build_rows(img, lhs, 1, 3)
        build_rows(img, lhs, SIDE, 3)
        build_strips(img, lhs, STRIPS[TWO:])


def operand(lhs, kind):
    tap, tail, strip = lhs
    runs, cut = kind
    blocks = []
    for dr in range(3):
        parts = [tap[er - 1 + dr:er - 1 + dr + n].reshape(n * SIDE, TAPS) for er, n in runs]
        blocks.append(parts + ([strip[dr, cut]] if cut else []))
    last = [tail[(er - 1) * SIDE:(er - 1 + n) * SIDE, :CH] for er, n in runs]
    if cut:
        last.append(tail[MAIN + cut.start:MAIN + cut.stop, :CH])
    return jnp.concatenate([jnp.concatenate(b, axis=0) for b in blocks + [last]], axis=1)


def conv(lhs, w, add, out, kind, first, parts):
    x = operand(lhs, kind)
    runs, cut = kind
    for p in parts:
        z = jnp.dot(x, w[:, TWO * p * L:TWO * (p + 1) * L], preferred_element_type=F32)
        for q in (TWO * p, TWO * p + 1):
            v = z[:, (q % TWO) * L:(q % TWO + 1) * L]

            def store(at, u):
                out[0][out[1], q, at, :] = u + (add[0][add[1], q, at, :] if isinstance(add, tuple) else add[q:q + 1, :])

            m = 0
            for er, n in runs:
                store(pl.ds((er - first) * SIDE, n * SIDE), v[m:m + n * SIDE])
                m += n * SIDE
            if cut and not cut.start:
                store(pl.ds(MAIN, TWO * STRIP), v[m:m + TWO * STRIP])
                m += TWO * STRIP
            if kind is EXT_OUT or kind is PLAIN_OUT:
                for side in range(TWO):
                    store(pl.ds((3 - first) * SIDE + 15 * side, INNER, stride=SIDE), v[m:m + INNER])
                    m += SIDE


def gates(z, c0, c1):
    lo = low_lanes(c0.shape[0])
    half = jnp.where(lo, 0.5, 1.0).astype(F32)
    off = jnp.where(lo, 0.5, 0.0).astype(F32)

    def sigmoid(v):
        return 0.5 * jnp.tanh(0.5 * v) + 0.5

    in0, a1, a2, out0 = [sigmoid(v) for v in z[:FOUR]]
    a4 = half * jnp.tanh(half * z[FOUR]) + off
    a5 = jnp.tanh(z[5])
    forget0 = pltpu.roll(jnp.where(lo, a2, a1), HALF, 1)
    cand0 = pltpu.roll(jnp.where(lo, a5, a4), HALF, 1)
    in_forget1 = jnp.where(lo, a1, a2)
    out_cand1 = jnp.where(lo, a4, a5)
    c0n = forget0 * c0 + in0 * cand0
    prod = in_forget1 * jnp.where(lo, pltpu.roll(out_cand1, HALF, 1), c1)
    c1n = prod + pltpu.roll(prod, HALF, 1)
    h0 = out0 * jnp.tanh(c0n)
    h1, _ = halves(out_cand1 * jnp.tanh(c1n))
    return h0.astype(BF), h1.astype(BF), c0n, c1n


def kernel(frames, w_x, w_h, bias_in, h_init, c_init, h_all, c_final,
           fr, hin, cin, bias_v, bias, wx, wh, imgx, imgh, cst, tapx, tailx, stripx, tapy, taily, stripy, taph, tailh, striph,
           gext, gpl, zext, zpl,
           s_xcol, s_xdiag, r_xrow, r_xcol, r_xdiag,
           s_hcol, s_ccol, s_diag, r_hrow, r_hcol, r_crow, r_ccol, r_diag,
           lsem, wsem, xs_sem, xr_sem, e_s, e_r, *, shape):
    lhs_x, lhs_y, lhs_h = (tapx, tailx, stripx), (tapy, taily, stripy), (taph, tailh, striph)
    n_rows, n_cols = shape
    row, col = lax.axis_index("rows"), lax.axis_index("cols")
    grp = lax.axis_index("batch")

    def has(d):
        dr, dc = DIRS[d]
        rr, cc = row + dr, col + dc
        return (rr >= 0) & (rr < n_rows) & (cc >= 0) & (cc < n_cols)

    def peer(d):
        return (grp, col + DIRS[d][1], row + DIRS[d][0])

    def each(dirs, ok, f):
        for d in dirs:
            @pl.when(ok(d))
            def _(d=d):
                f(d)

    load_h = pltpu.make_async_copy(h_init, hin, lsem.at[0])
    load_c = pltpu.make_async_copy(c_init, cin, lsem.at[1])
    load_b = pltpu.make_async_copy(bias_in, bias_v, lsem.at[TWO])
    load_f = [pltpu.make_async_copy(frames.at[pl.ds(TWO * k, TWO)], fr.at[pl.ds(TWO * k, TWO)], lsem.at[3 + k]) for k in range(FOUR)]
    load_w = [[], []]
    for i, (src, dst) in enumerate(((w_x, wx), (w_h, wh))):
        for dr in range(3):
            for dc in range(3):
                at = dr * TAPS + 3 * L + dc * HALF if dc < TWO else 3 * TAPS + dr * HALF
                for c_at, n, k_at in ((0, L, dr * TAPS + dc * L), (L, HALF, at)):
                    load_w[i].append(pltpu.make_async_copy(src.at[dr, dc, pl.ds(c_at, n)], dst.at[pl.ds(k_at, n)], wsem.at[i, len(load_w[i])]))
    for cp in [load_f[0], load_h, load_c, load_b] + load_w[0] + load_w[1] + load_f[1:]:
        cp.start()

    barrier = pltpu.get_barrier_semaphore()
    each(range(EIGHT), has, lambda d: pl.semaphore_signal(barrier, inc=1, device_id=peer(d), device_id_type=MESH))

    def blank(d):
        refs = (r_xrow, r_hrow, r_crow) if d < TWO else (r_xcol, r_hcol, r_ccol) if d < FOUR else (r_xdiag, r_diag)
        for ref in refs:
            ref[:, d % FOUR if d > 3 else d % TWO] = jnp.zeros((ref.shape[0],) + ref.shape[TWO:], ref.dtype)

    def frame_stage(k):
        for odd in range(TWO):
            for s in range(TWO):
                put_rows((imgx, FOUR * k + TWO * odd + s), TWO, fr[TWO * k + odd, s])
        for side in range(TWO):
            ec = (TWO + 15 * side, 3 + 13 * side)
            for s in range(TWO):
                img = (imgx, FOUR * k + s)
                pack_cols(s_xcol.at[TWO * k, side, s], *[get_col(img, lt, TWO, e) for e in ec for lt in range(TWO)])
            pack_cols(s_xcol.at[TWO * k + 1, side, 0], *[get_col((imgx, FOUR * k + TWO + s), lt, TWO, ec[0]) for s in range(TWO) for lt in range(TWO)])
        for d in range(FOUR, EIGHT):
            er, ec = [near(e) for e in corner_src(d)]
            for s in range(TWO):
                pack_corner(s_xdiag.at[k, d - FOUR, s], (imgx, FOUR * k + s), d, *[imgx[FOUR * k + TWO + s, lt, er, pl.ds(ec, 1), :] for lt in range(TWO)])

    def frame_copies(k, odd, d):
        f = TWO * k + odd

        def mk(src, dst):
            return [pltpu.make_async_remote_copy(src_ref=src, dst_ref=dst, send_sem=xs_sem.at[f, d], recv_sem=xr_sem.at[f, d], device_id=peer(d), device_id_type=MESH)]

        n = 1 if odd else TWO
        if d < TWO:
            at = SIDE - n if d else 0
            return mk(fr.at[f, :, pl.ds(at, n)], r_xrow.at[f, d, :, pl.ds(d if odd else 0, n)])
        if d < FOUR:
            return mk(s_xcol.at[f, d - TWO, pl.ds(0, n)], r_xcol.at[f, d - TWO, pl.ds(0, n)])
        return [] if odd else mk(s_xdiag.at[k, d - FOUR], r_xdiag.at[k, d - FOUR])

    def frame_send(k, odd):
        each(range(FOUR) if odd else (TWO, 3, FOUR, 5, 6, 7, 0, 1), has, lambda d: [cp.start() for cp in frame_copies(k, odd, d)])

    def frame_wait(k):
        each(range(EIGHT), lambda d: has(OPP[d]), lambda d: [cp.wait_recv() for odd in range(TWO) for cp in frame_copies(k, odd, d)])
        each(range(EIGHT), has, lambda d: [cp.wait_send() for odd in range(TWO) for cp in frame_copies(k, odd, d)])

    def frame_fill(k, odd, s):
        f = TWO * k + odd
        img = (imgx, TWO * f + s)
        for d in range(TWO):
            i, n = (d, 1) if odd else (0, TWO)
            put_rows(img, i + FAR * (1 - d), r_xrow[f, d, s, pl.ds(i, n)])
            ec = (1, 0) if d else (FAR, FAR + 1)
            if odd:
                b = halves(r_xcol[f, d, 0, TWO].astype(F32))
                b = b[s] if isinstance(s, int) else jnp.where(flag(s == 0, SIDE), *b)
                put_col(img, TWO, ec[0], r_xcol[f, d, 0, s].astype(F32), b)
            else:
                ab = unpack_cols(r_xcol[f, d, s])
                put_col(img, TWO, ec[0], *ab[:TWO])
                put_col(img, TWO, ec[1], *ab[TWO:])
        for d in range(FOUR, EIGHT):
            src = r_xdiag.at[k, d - FOUR, s]
            if odd:
                er, ec = [near(e) for e in corner_dst(d)]
                imgx[TWO * f + s, 0, er, pl.ds(ec, 1), :] = src[FOUR:5, :]
                imgx[TWO * f + s, 1, er, pl.ds(ec, 1), :] = src[7:EIGHT, :]
            else:
                unpack_corner(src, img, d)

    def x_build(k, odd, s, kind):
        build((imgx, FOUR * k + TWO * odd + s), lhs_y if odd else lhs_x, kind)

    def x_conv(s, odd, kind, parts=range(3)):
        conv(lhs_y if odd else lhs_x, wx, bias, (gpl if odd else gext, s), kind, 1 + odd, parts)

    def state_copies(e, s, d, hsrc, which=(0, 1)):
        x = TWO * e + s
        if d < TWO:
            refs = ((hsrc.at[pl.ds(INNER * d, TWO)], r_hrow.at[x, d]), (cst.at[s, :, pl.ds(SIDE + 240 * d, SIDE)], r_crow.at[x, d]))
        elif d < FOUR:
            refs = ((s_hcol.at[s, d - TWO], r_hcol.at[x, d - TWO]), (s_ccol.at[s, d - TWO], r_ccol.at[x, d - TWO]))
        else:
            refs = ((s_diag.at[s, d - FOUR], r_diag.at[x, d - FOUR]),)
        return [pltpu.make_async_remote_copy(src_ref=refs[i][0], dst_ref=refs[i][1], send_sem=e_s.at[x, d + EIGHT * i], recv_sem=e_r.at[x, d + EIGHT * i], device_id=peer(d), device_id_type=MESH) for i in which[:len(refs)]]

    def state_stage(s):
        img = (imgh, s)
        for side in range(TWO):
            ec = (TWO + 15 * side, 3 + 13 * side)
            pack_cols(s_hcol.at[s, side], *[get_col(img, lt, TWO, e) for e in ec for lt in range(TWO)])
            c0, c1 = [cst[s, lt, pl.ds(SIDE + 15 * side, SIDE, stride=SIDE), :] for lt in range(TWO)]
            s_ccol[s, side, :SIDE] = c0
            s_ccol[s, side, SIDE:] = join(c1[:EIGHT], c1[EIGHT:])
        for d in range(FOUR, EIGHT):
            er, ec = [near(e) for e in corner_src(d)]
            at = pl.ds((er - 1) * SIDE + ec - TWO, 1)
            pack_corner(s_diag.at[s, d - FOUR], img, d, cst[s, 0, at, :], cst[s, 1, at, :])

    def state_send(e, s, hsrc):
        each((TWO, 3, FOUR, 5, 6, 7, 0, 1), has, lambda d: state_copies(e, s, d, hsrc, (0,))[0].start())
        each(range(FOUR), has, lambda d: state_copies(e, s, d, hsrc, (1,))[0].start())

    def state_wait(e, s):
        each(range(EIGHT), lambda d: has(OPP[d]), lambda d: [cp.wait_recv() for cp in state_copies(e, s, d, hin.at[s])])
        each(range(EIGHT), has, lambda d: [cp.wait_send() for cp in state_copies(e, s, d, hin.at[s])])

    def state_fill(e, s):
        img = (imgh, s)
        x = TWO * e + s
        for d in range(TWO):
            put_rows(img, FAR * (1 - d), r_hrow[x, d])
            cst[s, :, pl.ds(272 * (1 - d), SIDE), :] = r_crow[x, d]
            ab = unpack_cols(r_hcol[x, d])
            ec = (1, 0) if d else (FAR, FAR + 1)
            put_col(img, TWO, ec[0], *ab[:TWO])
            put_col(img, TWO, ec[1], *ab[TWO:])
            v = r_ccol[x, d]
            m = MAIN + STRIP * (1 - d) + 1
            cst[s, 0, pl.ds(m, SIDE), :] = v[:SIDE]
            cst[s, 1, pl.ds(m, SIDE), :] = jnp.concatenate(halves(v[SIDE:]), axis=0)
        for d in range(FOUR, EIGHT):
            src = r_diag.at[x, d - FOUR]
            unpack_corner(src, img, d)
            er, ec = corner_dst(d)
            m = MAIN + (STRIP if ec else 0) + (17 if er else 0)
            cst[s, 0, pl.ds(m, 1), :] = src[FOUR:5, :]
            cst[s, 1, pl.ds(m, 1), :] = src[7:EIGHT, :]

    def flag(cond, n):
        return jnp.full((n, L), jnp.where(cond, 1, 0).astype(jnp.int32)) > 0

    def update(s, t, ext, last=False):
        img = (imgh, s)
        z_ref = zext if ext else zpl

        def one(m, n):
            zm = m if ext else m - SIDE
            z = [z_ref[s, p, zm:zm + n, :] for p in range(PIECES)]
            h0, h1, c0, c1 = gates(z, cst[s, 0, m:m + n, :], cst[s, 1, m:m + n, :])
            cst[s, 0, m:m + n, :] = c0
            cst[s, 1, m:m + n, :] = c1
            return h0, h1, c0, c1

        er, end = (1, FAR + 1) if ext else (TWO, FAR)
        while er < end:
            n = 1 if er == 1 or er == end - 1 else TWO
            h0, h1, c0, c1 = one((er - 1) * SIDE, n * SIDE)
            if 1 < er < FAR:
                at = pl.ds(er - TWO, n)
                h_all[t, s, at, :, :L] = h0.reshape(n, SIDE, L)
                h_all[t, s, at, :, L:] = h1[:, :HALF].reshape(n, SIDE, HALF)
            if last:
                c_final[s, at, :, :L] = c0.reshape(n, SIDE, L)
                c_final[s, at, :, L:] = c1[:, :HALF].reshape(n, SIDE, HALF)
            else:
                f0, f1 = h0.astype(F32), h1.astype(F32)
                if er == 1 or er == FAR:
                    ok = flag(has(er // FAR), n * SIDE)
                    f0, f1 = jnp.where(ok, f0, 0.0), jnp.where(ok, f1, 0.0)
                put_body(img, er, f0, f1)
            er += n
        if not ext:
            return
        pos = lax.broadcasted_iota(jnp.int32, (STRIP, L), 0)
        for side in range(TWO):
            ok = flag(has(TWO + side), STRIP) & (flag(has(0), STRIP) | (pos > 0)) & (flag(has(1), STRIP) | (pos < 17))
            h0, h1, _, _ = one(MAIN + STRIP * side, STRIP)
            put_col(img, 1, 1 + 17 * side, jnp.where(ok, h0.astype(F32), 0.0), jnp.where(ok, h1.astype(F32), 0.0))

    def h_build(s, kind):
        build((imgh, s), lhs_h, kind)

    def h_conv(s, kind):
        if kind is PLAIN:
            conv(lhs_h, wh, (gpl, s), (zpl, s), kind, TWO, range(3))
        else:
            conv(lhs_h, wh, (gext, s), (zext, s), kind, 1, range(3))

    load_f[0].wait()
    frame_stage(0)
    load_h.wait()
    load_c.wait()
    def first_state(s, _):
        put_rows((imgh, s), TWO, hin[s])
        v = cin[s].reshape(PLAIN_M, CH)
        at = pl.ds(SIDE, PLAIN_M)
        cst[s, 0, at, :] = v[:, :L]
        cst[s, 1, at, :] = twice(v[:, L:])
        state_stage(s)
        return 0

    lax.fori_loop(0, TWO, first_state, 0)
    near_rows = 1 + has(0).astype(jnp.int32) + has(1).astype(jnp.int32)
    near_cols = 1 + has(TWO).astype(jnp.int32) + has(3).astype(jnp.int32)
    pl.semaphore_wait(barrier, near_rows * near_cols - 1)
    frame_send(0, 0)
    frame_send(0, 1)

    def first_send(s, _):
        state_send(0, s, hin.at[s])
        return 0

    lax.fori_loop(0, TWO, first_send, 0)
    each(range(EIGHT), lambda d: jnp.logical_not(has(OPP[d])), blank)
    load_b.wait()
    for p in range(PIECES):
        bias[p:p + 1, :] = bias_v[pl.ds(p * L, L)].reshape(1, L)
    for cp in load_w[0]:
        cp.wait()
    def first_x(s, _):
        for odd in range(TWO):
            x_build(0, odd, s, IN)
            x_conv(s, odd, IN)
        return 0

    lax.fori_loop(0, TWO, first_x, 0)
    for cp in load_w[1] + load_f[1:]:
        cp.wait()

    def stage_body(k, _):
        frame_stage(k)
        frame_send(k, 0)
        frame_send(k, 1)
        return 0

    lax.fori_loop(1, FOUR, stage_body, 0)
    def first_h(s, _):
        h_build(s, IN)
        h_conv(s, IN)
        return 0

    def first_border(s, _):
        for odd in range(TWO):
            kind = PLAIN_OUT if odd else EXT_OUT
            frame_fill(0, odd, s)
            x_build(0, odd, s, kind)
            x_conv(s, odd, kind)
        return 0

    lax.fori_loop(0, TWO, first_h, 0)
    frame_wait(0)
    lax.fori_loop(0, TWO, first_border, 0)

    def round_body(k, _):
        frame_wait(k + 1)
        for s in range(TWO):
            state_wait(k, s)
            state_fill(k, s)
            h_build(s, EXT_OUT)
            h_conv(s, EXT_OUT)
            frame_fill(k + 1, 0, s)
            x_build(k + 1, 0, s, EXT)
            x_conv(s, 0, EXT, (0, 1))
            update(s, TWO * k, True)
            h_build(s, PLAIN)
            h_conv(s, PLAIN)
            frame_fill(k + 1, 1, s)
            x_build(k + 1, 1, s, PLAIN)
            x_conv(s, 0, EXT, (TWO,))
            x_conv(s, 1, PLAIN, (0,))
            update(s, TWO * k + 1, False)
            state_stage(s)
            state_send(k + 1, s, h_all.at[TWO * k + 1, s])
            h_build(s, IN)
            x_conv(s, 1, PLAIN, (1, TWO))
            h_conv(s, IN)
        return 0

    lax.fori_loop(0, 3, round_body, 0)
    last = 3
    for s in range(TWO):
        state_wait(last, s)
        state_fill(last, s)
        h_build(s, EXT_OUT)
        h_conv(s, EXT_OUT)
        if s == 0:
            update(0, TWO * last, True)
    h_build(0, PLAIN)
    h_conv(0, PLAIN)
    update(1, TWO * last, True)
    h_build(1, PLAIN)
    update(0, TWO * last + 1, False, True)
    h_conv(1, PLAIN)
    update(1, TWO * last + 1, False, True)


def solution(mesh):
    shape = (mesh.shape["rows"], mesh.shape["cols"])
    frame_spec = P(None, "batch", "rows", "cols", None)
    state_spec = P("batch", "rows", "cols", None)
    any_spec = pl.BlockSpec(memory_space=pl.ANY)
    vmem = pl.BlockSpec(memory_space=pltpu.VMEM)

    def local_run(frames, w_x, w_h, gate_bias, h_init, c_init):
        V = pltpu.VMEM
        D = pltpu.SemaphoreType.DMA
        lhs = [V((20, SIDE, TAPS), BF), V((MAIN + STRIP_M, TWO * L), BF), V((3, STRIP_M, TAPS), BF)]
        pair = (TWO, TWO)
        scratch = [
            V(frames.shape, BF), V(h_init.shape, BF), V(c_init.shape, F32), V(gate_bias.shape, F32), V((EIGHT, L), F32),
            V((9 * CH, GATES), BF), V((9 * CH, GATES), BF),
            V((SIDE, TWO, IMG_ROWS, PITCH, L), F32), V(pair + (IMG_ROWS, PITCH, L), F32), V(pair + (EXT_M, L), F32),
            *lhs, *lhs, *lhs,
            V((TWO, PIECES, EXT_M, L), F32), V((TWO, PIECES, PLAIN_M, L), F32), V((TWO, PIECES, EXT_M, L), F32), V((TWO, PIECES, PLAIN_M, L), F32),
            V((EIGHT, TWO, TWO, 3, SIDE, L), BF), V((FOUR, FOUR, TWO, EIGHT, L), F32),
            V((EIGHT, TWO, TWO, TWO, SIDE, CH), BF), V((EIGHT, TWO, TWO, 3, SIDE, L), BF), V((FOUR, FOUR, TWO, EIGHT, L), F32),
            V(pair + (3, SIDE, L), BF), V(pair + (STRIP, L), F32), V((TWO, FOUR, EIGHT, L), F32),
            V((EIGHT, TWO, TWO, SIDE, CH), BF), V((EIGHT, TWO, 3, SIDE, L), BF), V((EIGHT, TWO, TWO, SIDE, L), F32), V((EIGHT, TWO, STRIP, L), F32), V((EIGHT, FOUR, EIGHT, L), F32),
            D((7,)), D((TWO, FAR)), D((EIGHT, EIGHT)), D((EIGHT, EIGHT)), D((EIGHT, 12)), D((EIGHT, 12)),
        ]
        return pl.pallas_call(
            functools.partial(kernel, shape=shape),
            out_shape=[V(frames.shape, BF), V(c_init.shape, F32)],
            in_specs=[any_spec] * 6,
            out_specs=[vmem, vmem],
            scratch_shapes=scratch,
            compiler_params=pltpu.CompilerParams(collective_id=0, has_side_effects=True, vmem_limit_bytes=60 * 1024 * 1024),
            name="convlstm",
        )(frames, w_x, w_h, gate_bias, h_init, c_init)

    return jax.shard_map(local_run, mesh=mesh, in_specs=(frame_spec, P(), P(), P(), state_spec, state_spec), out_specs=(frame_spec, state_spec), check_vma=False)
```

```python
import functools

import jax
import jax.numpy as jnp
from jax import lax
from jax.experimental import pallas as pl
from jax.experimental.pallas import tpu as pltpu
from jax.sharding import PartitionSpec as P

MESH = pl.DeviceIdType.MESH
BF = jnp.bfloat16
F32 = jnp.float32

L, HALF, SIDE, CH, GATES, TAPS = 128, 64, 16, 192, 768, 512
TWO, FOUR, EIGHT, FAR = 2, 4, 8, 18
PIECES = 6
PITCH = 24
IMG_ROWS = 26
STRIP = 24
MAIN = 288
EXT_M = 336
PLAIN_M = 256
INNER = 14
DIRS = ((-1, 0), (1, 0), (0, -1), (0, 1), (-1, -1), (-1, 1), (1, -1), (1, 1))
OPP = (1, 0, 3, 2, 7, 6, 5, 4)
STRIPS = ((1, 1, STRIP), (FAR, 1, STRIP), (2, 3, SIDE), (17, 3, SIDE))
STRIP_M = 80
EXT = (((1, FAR),), slice(0, 48))
PLAIN = (((2, SIDE),), None)
IN = (((3, INNER),), None)
EXT_OUT = (((1, 2), (17, 2)), slice(0, STRIP_M))
PLAIN_OUT = (((2, 1), (17, 1)), slice(48, STRIP_M))


def cell(er, ec):
    return er * PITCH + ec


def corner_src(d):
    return (TWO if DIRS[d][0] < 0 else SIDE), (TWO if DIRS[d][1] < 0 else SIDE)


def corner_dst(d):
    return (FAR if DIRS[d][0] < 0 else 0), (FAR if DIRS[d][1] < 0 else 0)


def near(e):
    return {TWO: TWO, SIDE: 17, FAR: FAR, 0: 1}[e]


def low_lanes(n):
    return lax.broadcasted_iota(jnp.int32, (n, L), 1) < HALF


def twice(v):
    return jnp.concatenate([v, v], axis=1)


def halves(v):
    lo, w = low_lanes(v.shape[0]), pltpu.roll(v, HALF, 1)
    return jnp.where(lo, v, w), jnp.where(lo, w, v)


def join(a, b):
    return jnp.where(low_lanes(a.shape[0]), a, b)


def flat(ref):
    return ref.reshape(ref.shape[0], TWO, IMG_ROWS * PITCH, L)


def put_col(img, er, ec, a, b):
    ref, x = img
    at = pl.ds(cell(er, ec), a.shape[0], stride=PITCH)
    flat(ref)[x, 0, at, :] = a
    flat(ref)[x, 1, at, :] = b


def get_col(img, lt, er, ec, n=SIDE):
    ref, x = img
    return flat(ref)[x, lt, pl.ds(cell(er, ec), n, stride=PITCH), :]


def put_rows(img, er, v):
    n = v.shape[0]
    v = v.reshape(n * SIDE, CH).astype(F32)
    put_body(img, er, v[:, :L], twice(v[:, L:]))


def put_body(img, er, a, b):
    n = a.shape[0] // SIDE
    ref, x = img
    for lt, v in enumerate((a, b)):
        ref[x, lt, pl.ds(er, n), TWO:FAR, :] = v.reshape(n, SIDE, L)


def pack_cols(dst, a0, b0, a1, b1):
    for i, v in enumerate((a0, a1, join(b0, b1))):
        dst[i] = v.astype(dst.dtype)


def unpack_cols(src):
    b0, b1 = halves(src[TWO].astype(F32))
    return src[0].astype(F32), b0, src[1].astype(F32), b1


def pack_corner(dst, img, d, a, b):
    er, ec = corner_src(d)
    ref, x = img
    for i in range(TWO):
        dst[TWO * i:TWO * i + TWO, :] = ref[x, 0, er + i, pl.ds(ec, TWO), :]
        dst[5 + i:6 + i, :] = join(ref[x, 1, er + i, pl.ds(ec, 1), :], ref[x, 1, er + i, pl.ds(ec + 1, 1), :])
    dst[FOUR:5, :] = a
    dst[7:EIGHT, :] = b


def unpack_corner(src, img, d):
    er, ec = corner_dst(d)
    ref, x = img
    for i in range(TWO):
        ref[x, 0, er + i, pl.ds(ec, TWO), :] = src[TWO * i:TWO * i + TWO, :]
        for j, v in enumerate(halves(src[5 + i:6 + i, :])):
            ref[x, 1, er + i, pl.ds(ec + j, 1), :] = v


def build_rows(img, lhs, first, n):
    tap, tail, _ = lhs
    ref, x = img
    rows = slice(first, first + n)
    lo = lax.broadcasted_iota(jnp.int32, (n, SIDE, L), TWO) < HALF
    for dc in range(3):
        tap[rows, :, dc * L:(dc + 1) * L] = ref[x, 0, rows, 1 + dc:17 + dc, :].astype(BF)
    b = [ref[x, 1, rows, 1 + dc:17 + dc, :] for dc in range(3)]
    tap[rows, :, 3 * L:] = jnp.where(lo, b[0], b[1]).astype(BF)
    m = n - TWO
    at = pl.ds(first * SIDE, m * SIDE)
    tail[at, :L] = jnp.where(lo[:m], b[TWO][:m], b[TWO][1:n - 1]).astype(BF).reshape(m * SIDE, L)
    tail[at, L:] = b[TWO][TWO:].astype(BF).reshape(m * SIDE, L)


def build_strips(img, lhs, which):
    _, tail, strip = lhs
    at = 0
    for ec, er, n in STRIPS:
        rows = slice(at, at + n)
        at += n
        if (ec, er, n) not in which:
            continue

        def col(lt, dr, dc):
            return get_col(img, lt, er - 1 + dr, ec - 1 + dc, n)

        for dr in range(3):
            for dc in range(3):
                strip[dr, rows, dc * L:(dc + 1) * L] = col(0, dr, dc).astype(BF)
            strip[dr, rows, 3 * L:] = join(col(1, dr, 0), col(1, dr, 1)).astype(BF)
        rows = slice(MAIN + rows.start, MAIN + rows.stop)
        tail[rows, :L] = join(col(1, 0, TWO), col(1, 1, TWO)).astype(BF)
        tail[rows, L:] = col(1, TWO, TWO).astype(BF)


def build(img, lhs, kind):
    if kind is EXT:
        build_rows(img, lhs, 0, 20)
        build_strips(img, lhs, STRIPS[:TWO])
    elif kind is PLAIN:
        build_rows(img, lhs, 1, FAR)
    elif kind is IN:
        build_rows(img, lhs, TWO, SIDE)
    elif kind is EXT_OUT:
        build_rows(img, lhs, 0, FOUR)
        build_rows(img, lhs, SIDE, FOUR)
        build_strips(img, lhs, STRIPS)
    else:
        build_rows(img, lhs, 1, 3)
        build_rows(img, lhs, SIDE, 3)
        build_strips(img, lhs, STRIPS[TWO:])


def operand(lhs, kind):
    tap, tail, strip = lhs
    runs, cut = kind
    blocks = []
    for dr in range(3):
        parts = [tap[er - 1 + dr:er - 1 + dr + n].reshape(n * SIDE, TAPS) for er, n in runs]
        blocks.append(parts + ([strip[dr, cut]] if cut else []))
    last = [tail[(er - 1) * SIDE:(er - 1 + n) * SIDE, :CH] for er, n in runs]
    if cut:
        last.append(tail[MAIN + cut.start:MAIN + cut.stop, :CH])
    return jnp.concatenate([jnp.concatenate(b, axis=0) for b in blocks + [last]], axis=1)


def conv(lhs, w, add, out, kind, first, parts):
    x = operand(lhs, kind)
    runs, cut = kind
    for p in parts:
        z = jnp.dot(x, w[:, TWO * p * L:TWO * (p + 1) * L], preferred_element_type=F32)
        for q in (TWO * p, TWO * p + 1):
            v = z[:, (q % TWO) * L:(q % TWO + 1) * L]

            def store(at, u):
                out[0][out[1], q, at, :] = u + (add[0][add[1], q, at, :] if isinstance(add, tuple) else add[q:q + 1, :])

            m = 0
            for er, n in runs:
                store(pl.ds((er - first) * SIDE, n * SIDE), v[m:m + n * SIDE])
                m += n * SIDE
            if cut and not cut.start:
                store(pl.ds(MAIN, TWO * STRIP), v[m:m + TWO * STRIP])
                m += TWO * STRIP
            if kind is EXT_OUT or kind is PLAIN_OUT:
                for side in range(TWO):
                    store(pl.ds((3 - first) * SIDE + 15 * side, INNER, stride=SIDE), v[m:m + INNER])
                    m += SIDE


def gates(z, c0, c1):
    lo = low_lanes(c0.shape[0])
    half = jnp.where(lo, 0.5, 1.0).astype(F32)
    off = jnp.where(lo, 0.5, 0.0).astype(F32)

    def sigmoid(v):
        return 0.5 * jnp.tanh(0.5 * v) + 0.5

    in0, a1, a2, out0 = [sigmoid(v) for v in z[:FOUR]]
    a4 = half * jnp.tanh(half * z[FOUR]) + off
    a5 = jnp.tanh(z[5])
    forget0 = pltpu.roll(jnp.where(lo, a2, a1), HALF, 1)
    cand0 = pltpu.roll(jnp.where(lo, a5, a4), HALF, 1)
    in_forget1 = jnp.where(lo, a1, a2)
    out_cand1 = jnp.where(lo, a4, a5)
    c0n = forget0 * c0 + in0 * cand0
    prod = in_forget1 * jnp.where(lo, pltpu.roll(out_cand1, HALF, 1), c1)
    c1n = prod + pltpu.roll(prod, HALF, 1)
    h0 = out0 * jnp.tanh(c0n)
    h1, _ = halves(out_cand1 * jnp.tanh(c1n))
    return h0.astype(BF), h1.astype(BF), c0n, c1n


def kernel(frames, w_x, w_h, bias_in, h_init, c_init, h_all, c_final,
           fr, hin, cin, bias_v, bias, wx, wh, imgx, imgh, cst, tapx, tailx, stripx, tapy, taily, stripy, taph, tailh, striph, tapi, taili,
           gext, gpl, zext, zpl,
           s_xcol, s_xdiag, r_xrow, r_xcol, r_xdiag,
           s_hcol, s_ccol, s_diag, r_hrow, r_hcol, r_crow, r_ccol, r_diag,
           lsem, wsem, xs_sem, xr_sem, e_s, e_r, *, shape):
    lhs_x, lhs_y, lhs_h, lhs_i = (tapx, tailx, stripx), (tapy, taily, stripy), (taph, tailh, striph), (tapi, taili, None)
    n_rows, n_cols = shape
    row, col = lax.axis_index("rows"), lax.axis_index("cols")
    grp = lax.axis_index("batch")

    def has(d):
        dr, dc = DIRS[d]
        rr, cc = row + dr, col + dc
        return (rr >= 0) & (rr < n_rows) & (cc >= 0) & (cc < n_cols)

    def peer(d):
        return (grp, col + DIRS[d][1], row + DIRS[d][0])

    have = [has(d) for d in range(EIGHT)]

    def each(f, dirs=(TWO, 3, FOUR, 5, 6, 7, 0, 1)):
        for d in dirs:
            @pl.when(have[d])
            def _(d=d):
                f(d)

    def start(copies):
        for cp in copies:
            cp.start()

    def exchanged(copies, d):
        for cp in copies(OPP[d]):
            cp.wait_recv()
        for cp in copies(d):
            cp.wait_send()

    load_h = pltpu.make_async_copy(h_init, hin, lsem.at[0])
    load_c = pltpu.make_async_copy(c_init, cin, lsem.at[1])
    load_b = pltpu.make_async_copy(bias_in, bias_v, lsem.at[TWO])
    load_f = [pltpu.make_async_copy(frames.at[pl.ds(TWO * k, TWO)], fr.at[pl.ds(TWO * k, TWO)], lsem.at[3 + k]) for k in range(FOUR)]
    load_w = [[], []]
    for i, (src, dst) in enumerate(((w_x, wx), (w_h, wh))):
        for dr in range(3):
            for dc in range(3):
                at = dr * TAPS + 3 * L + dc * HALF if dc < TWO else 3 * TAPS + dr * HALF
                for c_at, n, k_at in ((0, L, dr * TAPS + dc * L), (L, HALF, at)):
                    load_w[i].append(pltpu.make_async_copy(src.at[dr, dc, pl.ds(c_at, n)], dst.at[pl.ds(k_at, n)], wsem.at[i, len(load_w[i])]))
    start([load_f[0], load_h, load_c, load_b] + load_w[0])

    barrier = pltpu.get_barrier_semaphore()
    each(lambda d: pl.semaphore_signal(barrier, inc=1, device_id=peer(d), device_id_type=MESH))

    def blank(d):
        refs = (r_xrow, r_hrow, r_crow) if d < TWO else (r_xcol, r_hcol, r_ccol) if d < FOUR else (r_xdiag, r_diag)
        for ref in refs:
            ref[:, d % FOUR if d > 3 else d % TWO] = jnp.zeros((ref.shape[0],) + ref.shape[TWO:], ref.dtype)

    def frame_stage(k):
        for odd in range(TWO):
            for s in range(TWO):
                put_rows((imgx, FOUR * k + TWO * odd + s), TWO, fr[TWO * k + odd, s])
        for side in range(TWO):
            ec = (TWO + 15 * side, 3 + 13 * side)
            for s in range(TWO):
                img = (imgx, FOUR * k + s)
                pack_cols(s_xcol.at[TWO * k, side, s], *[get_col(img, lt, TWO, e) for e in ec for lt in range(TWO)])
            pack_cols(s_xcol.at[TWO * k + 1, side, 0], *[get_col((imgx, FOUR * k + TWO + s), lt, TWO, ec[0]) for s in range(TWO) for lt in range(TWO)])
        for d in range(FOUR, EIGHT):
            er, ec = [near(e) for e in corner_src(d)]
            for s in range(TWO):
                pack_corner(s_xdiag.at[k, d - FOUR, s], (imgx, FOUR * k + s), d, *[imgx[FOUR * k + TWO + s, lt, er, pl.ds(ec, 1), :] for lt in range(TWO)])

    def frame_copies(k, odd, d):
        f = TWO * k + odd

        def mk(src, dst):
            return [pltpu.make_async_remote_copy(src_ref=src, dst_ref=dst, send_sem=xs_sem.at[f, d], recv_sem=xr_sem.at[f, d], device_id=peer(d), device_id_type=MESH)]

        n = 1 if odd else TWO
        if d < TWO:
            at = SIDE - n if d else 0
            return mk(fr.at[f, :, pl.ds(at, n)], r_xrow.at[f, d, :, pl.ds(d if odd else 0, n)])
        if d < FOUR:
            return mk(s_xcol.at[f, d - TWO, pl.ds(0, n)], r_xcol.at[f, d - TWO, pl.ds(0, n)])
        return [] if odd else mk(s_xdiag.at[k, d - FOUR], r_xdiag.at[k, d - FOUR])

    def both_frames(k):
        return lambda d: frame_copies(k, 0, d) + frame_copies(k, 1, d)

    def frame_wait(k):
        each(lambda d: exchanged(both_frames(k), d))

    def frame_fill(k, odd, s):
        f = TWO * k + odd
        img = (imgx, TWO * f + s)
        for d in range(TWO):
            i, n = (d, 1) if odd else (0, TWO)
            put_rows(img, i + FAR * (1 - d), r_xrow[f, d, s, pl.ds(i, n)])
            ec = (1, 0) if d else (FAR, FAR + 1)
            if odd:
                b = halves(r_xcol[f, d, 0, TWO].astype(F32))
                b = b[s] if isinstance(s, int) else jnp.where(flag(s == 0, SIDE), *b)
                put_col(img, TWO, ec[0], r_xcol[f, d, 0, s].astype(F32), b)
            else:
                ab = unpack_cols(r_xcol[f, d, s])
                put_col(img, TWO, ec[0], *ab[:TWO])
                put_col(img, TWO, ec[1], *ab[TWO:])
        for d in range(FOUR, EIGHT):
            src = r_xdiag.at[k, d - FOUR, s]
            if odd:
                er, ec = [near(e) for e in corner_dst(d)]
                imgx[TWO * f + s, 0, er, pl.ds(ec, 1), :] = src[FOUR:5, :]
                imgx[TWO * f + s, 1, er, pl.ds(ec, 1), :] = src[7:EIGHT, :]
            else:
                unpack_corner(src, img, d)

    def x_build(k, odd, s, kind):
        build((imgx, FOUR * k + TWO * odd + s), lhs_y if odd else lhs_x, kind)

    def x_conv(s, odd, kind, parts=range(3)):
        conv(lhs_y if odd else lhs_x, wx, bias, (gpl if odd else gext, s), kind, 1 + odd, parts)

    def state_copies(e, s, d, hsrc):
        x = TWO * e + s
        if d < TWO:
            refs = ((hsrc.at[pl.ds(INNER * d, TWO)], r_hrow.at[x, d]), (cst.at[s, :, pl.ds(SIDE + 240 * d, SIDE)], r_crow.at[x, d]))
        elif d < FOUR:
            refs = ((s_hcol.at[s, d - TWO], r_hcol.at[x, d - TWO]), (s_ccol.at[s, d - TWO], r_ccol.at[x, d - TWO]))
        else:
            refs = ((s_diag.at[s, d - FOUR], r_diag.at[x, d - FOUR]),)
        return [pltpu.make_async_remote_copy(src_ref=refs[i][0], dst_ref=refs[i][1], send_sem=e_s.at[x, d + EIGHT * i], recv_sem=e_r.at[x, d + EIGHT * i], device_id=peer(d), device_id_type=MESH) for i in range(len(refs))]

    def state_stage(s):
        img = (imgh, s)
        for side in range(TWO):
            ec = (TWO + 15 * side, 3 + 13 * side)
            pack_cols(s_hcol.at[s, side], *[get_col(img, lt, TWO, e) for e in ec for lt in range(TWO)])
            c0, c1 = [cst[s, lt, pl.ds(SIDE + 15 * side, SIDE, stride=SIDE), :] for lt in range(TWO)]
            s_ccol[s, side, :SIDE] = c0
            s_ccol[s, side, SIDE:] = join(c1[:EIGHT], c1[EIGHT:])
        for d in range(FOUR, EIGHT):
            er, ec = [near(e) for e in corner_src(d)]
            at = pl.ds((er - 1) * SIDE + ec - TWO, 1)
            pack_corner(s_diag.at[s, d - FOUR], img, d, cst[s, 0, at, :], cst[s, 1, at, :])

    def state_send(e, s, hsrc):
        each(lambda d: start(state_copies(e, s, d, hsrc)))

    def state_wait(e, s):
        each(lambda d: exchanged(lambda d: state_copies(e, s, d, hin.at[s]), d))

    def state_fill(e, s):
        img = (imgh, s)
        x = TWO * e + s
        for d in range(TWO):
            put_rows(img, FAR * (1 - d), r_hrow[x, d])
            cst[s, :, pl.ds(272 * (1 - d), SIDE), :] = r_crow[x, d]
            ab = unpack_cols(r_hcol[x, d])
            ec = (1, 0) if d else (FAR, FAR + 1)
            put_col(img, TWO, ec[0], *ab[:TWO])
            put_col(img, TWO, ec[1], *ab[TWO:])
            v = r_ccol[x, d]
            m = MAIN + STRIP * (1 - d) + 1
            cst[s, 0, pl.ds(m, SIDE), :] = v[:SIDE]
            cst[s, 1, pl.ds(m, SIDE), :] = jnp.concatenate(halves(v[SIDE:]), axis=0)
        for d in range(FOUR, EIGHT):
            src = r_diag.at[x, d - FOUR]
            unpack_corner(src, img, d)
            er, ec = corner_dst(d)
            m = MAIN + (STRIP if ec else 0) + (17 if er else 0)
            cst[s, 0, pl.ds(m, 1), :] = src[FOUR:5, :]
            cst[s, 1, pl.ds(m, 1), :] = src[7:EIGHT, :]

    def at_side(d):
        return have[d]

    def flag(cond, n):
        return jnp.full((n, L), jnp.where(cond, 1, 0).astype(jnp.int32)) > 0

    def update(s, t, ext, last=False):
        img = (imgh, s)
        z_ref = zext if ext else zpl

        def one(m, n):
            zm = m if ext else m - SIDE
            z = [z_ref[s, p, zm:zm + n, :] for p in range(PIECES)]
            h0, h1, c0, c1 = gates(z, cst[s, 0, m:m + n, :], cst[s, 1, m:m + n, :])
            cst[s, 0, m:m + n, :] = c0
            cst[s, 1, m:m + n, :] = c1
            return h0, h1, c0, c1

        er, end = (1, FAR + 1) if ext else (TWO, FAR)
        while er < end:
            n = 1 if er == 1 or er == end - 1 else TWO
            h0, h1, c0, c1 = one((er - 1) * SIDE, n * SIDE)
            if 1 < er < FAR:
                at = pl.ds(er - TWO, n)
                h_all[t, s, at, :, :L] = h0.reshape(n, SIDE, L)
                h_all[t, s, at, :, L:] = h1[:, :HALF].reshape(n, SIDE, HALF)
            if last:
                c_final[s, at, :, :L] = c0.reshape(n, SIDE, L)
                c_final[s, at, :, L:] = c1[:, :HALF].reshape(n, SIDE, HALF)
            else:
                f0, f1 = h0.astype(F32), h1.astype(F32)
                if er == 1 or er == FAR:
                    ok = flag(at_side(er // FAR), n * SIDE)
                    f0, f1 = jnp.where(ok, f0, 0.0), jnp.where(ok, f1, 0.0)
                put_body(img, er, f0, f1)
            er += n
        if not ext:
            return
        pos = lax.broadcasted_iota(jnp.int32, (STRIP, L), 0)
        for side in range(TWO):
            ok = flag(at_side(TWO + side), STRIP) & (flag(at_side(0), STRIP) | (pos > 0)) & (flag(at_side(1), STRIP) | (pos < 17))
            h0, h1, _, _ = one(MAIN + STRIP * side, STRIP)
            put_col(img, 1, 1 + 17 * side, jnp.where(ok, h0.astype(F32), 0.0), jnp.where(ok, h1.astype(F32), 0.0))

    def h_build(s, kind):
        build((imgh, s), lhs_i if kind is IN else lhs_h, kind)

    def h_conv(s, kind):
        if kind is PLAIN:
            conv(lhs_h, wh, (gpl, s), (zpl, s), kind, TWO, range(3))
        else:
            conv(lhs_i if kind is IN else lhs_h, wh, (gext, s), (zext, s), kind, 1, range(3))

    load_f[0].wait()
    frame_stage(0)
    load_h.wait()
    load_c.wait()
    def first_state(s, _):
        put_rows((imgh, s), TWO, hin[s])
        v = cin[s].reshape(PLAIN_M, CH)
        at = pl.ds(SIDE, PLAIN_M)
        cst[s, 0, at, :] = v[:, :L]
        cst[s, 1, at, :] = twice(v[:, L:])
        state_stage(s)
        return 0

    lax.fori_loop(0, TWO, first_state, 0)
    near_rows = 1 + have[0].astype(jnp.int32) + have[1].astype(jnp.int32)
    near_cols = 1 + have[TWO].astype(jnp.int32) + have[3].astype(jnp.int32)
    pl.semaphore_wait(barrier, near_rows * near_cols - 1)
    each(lambda d: start(frame_copies(0, 0, d) + state_copies(0, 0, d, hin.at[0]) + frame_copies(0, 1, d) + state_copies(0, 1, d, hin.at[1])))
    start(load_w[1] + load_f[1:])
    for d in range(EIGHT):
        @pl.when(jnp.logical_not(have[OPP[d]]))
        def _(d=d):
            blank(d)
    load_b.wait()
    for p in range(PIECES):
        bias[p:p + 1, :] = bias_v[pl.ds(p * L, L)].reshape(1, L)
    for cp in load_w[0]:
        cp.wait()
    for s in range(TWO):
        for odd in range(TWO - s):
            x_build(0, odd, s, IN)
            x_conv(s, odd, IN)
    for cp in load_w[1] + load_f[1:]:
        cp.wait()

    def stage_body(k, _):
        frame_stage(k)
        each(lambda d: start(both_frames(k)(d)))
        return 0

    lax.fori_loop(1, FOUR, stage_body, 0)
    h_build(0, IN)
    h_conv(0, IN)
    frame_wait(0)
    for s in range(TWO):
        for odd in range(TWO):
            kind = (PLAIN if s else PLAIN_OUT) if odd else EXT_OUT
            frame_fill(0, odd, s)
            x_build(0, odd, s, kind)
            x_conv(s, odd, kind, (0,) if kind is PLAIN else range(3))

    def left_over(s):
        x_conv(s, 1, PLAIN, (1, TWO))
        h_build(s, IN)
        h_conv(s, IN)

    def round_body(k, _):
        frame_wait(k + 1)
        for s in range(TWO):
            state_wait(k, s)
            left_over(1 - s)
            state_fill(k, s)
            h_build(s, EXT_OUT)
            h_conv(s, EXT_OUT)
            frame_fill(k + 1, 0, s)
            x_build(k + 1, 0, s, EXT)
            x_conv(s, 0, EXT, (0, 1))
            update(s, TWO * k, True)
            h_build(s, PLAIN)
            h_conv(s, PLAIN)
            frame_fill(k + 1, 1, s)
            x_build(k + 1, 1, s, PLAIN)
            x_conv(s, 0, EXT, (TWO,))
            x_conv(s, 1, PLAIN, (0,))
            update(s, TWO * k + 1, False)
            state_stage(s)
            state_send(k + 1, s, h_all.at[TWO * k + 1, s])
        return 0

    lax.fori_loop(0, 3, round_body, 0)
    last = 3
    for s in range(TWO):
        state_wait(last, s)
        if s == 0:
            left_over(1)
        state_fill(last, s)
        h_build(s, EXT_OUT)
        h_conv(s, EXT_OUT)
        if s == 0:
            update(0, TWO * last, True)
    h_build(0, PLAIN)
    h_conv(0, PLAIN)
    update(1, TWO * last, True)
    h_build(1, PLAIN)
    update(0, TWO * last + 1, False, True)
    h_conv(1, PLAIN)
    update(1, TWO * last + 1, False, True)


def solution(mesh):
    shape = (mesh.shape["rows"], mesh.shape["cols"])
    frame_spec = P(None, "batch", "rows", "cols", None)
    state_spec = P("batch", "rows", "cols", None)
    any_spec = pl.BlockSpec(memory_space=pl.ANY)
    vmem = pl.BlockSpec(memory_space=pltpu.VMEM)

    def local_run(frames, w_x, w_h, gate_bias, h_init, c_init):
        V = pltpu.VMEM
        D = pltpu.SemaphoreType.DMA
        lhs = [V((20, SIDE, TAPS), BF), V((MAIN + STRIP_M, TWO * L), BF), V((3, STRIP_M, TAPS), BF)]
        pair = (TWO, TWO)
        scratch = [
            V(frames.shape, BF), V(h_init.shape, BF), V(c_init.shape, F32), V(gate_bias.shape, F32), V((EIGHT, L), F32),
            V((9 * CH, GATES), BF), V((9 * CH, GATES), BF),
            V((SIDE, TWO, IMG_ROWS, PITCH, L), F32), V(pair + (IMG_ROWS, PITCH, L), F32), V(pair + (EXT_M, L), F32),
            *lhs, *lhs, *lhs, *lhs[:TWO],
            V((TWO, PIECES, EXT_M, L), F32), V((TWO, PIECES, PLAIN_M, L), F32), V((TWO, PIECES, EXT_M, L), F32), V((TWO, PIECES, PLAIN_M, L), F32),
            V((EIGHT, TWO, TWO, 3, SIDE, L), BF), V((FOUR, FOUR, TWO, EIGHT, L), F32),
            V((EIGHT, TWO, TWO, TWO, SIDE, CH), BF), V((EIGHT, TWO, TWO, 3, SIDE, L), BF), V((FOUR, FOUR, TWO, EIGHT, L), F32),
            V(pair + (3, SIDE, L), BF), V(pair + (STRIP, L), F32), V((TWO, FOUR, EIGHT, L), F32),
            V((EIGHT, TWO, TWO, SIDE, CH), BF), V((EIGHT, TWO, 3, SIDE, L), BF), V((EIGHT, TWO, TWO, SIDE, L), F32), V((EIGHT, TWO, STRIP, L), F32), V((EIGHT, FOUR, EIGHT, L), F32),
            D((7,)), D((TWO, FAR)), D((EIGHT, EIGHT)), D((EIGHT, EIGHT)), D((EIGHT, 12)), D((EIGHT, 12)),
        ]
        return pl.pallas_call(
            functools.partial(kernel, shape=shape),
            out_shape=[V(frames.shape, BF), V(c_init.shape, F32)],
            in_specs=[any_spec] * 6,
            out_specs=[vmem, vmem],
            scratch_shapes=scratch,
            compiler_params=pltpu.CompilerParams(collective_id=0, has_side_effects=True, vmem_limit_bytes=60 * 1024 * 1024),
            name="convlstm",
        )(frames, w_x, w_h, gate_bias, h_init, c_init)

    return jax.shard_map(local_run, mesh=mesh, in_specs=(frame_spec, P(), P(), P(), state_spec, state_spec), out_specs=(frame_spec, state_spec), check_vma=False)
```

```python
import functools

import jax
import jax.numpy as jnp
from jax import lax
from jax.experimental import pallas as pl
from jax.experimental.pallas import tpu as pltpu
from jax.sharding import PartitionSpec as P

MESH = pl.DeviceIdType.MESH
BF = jnp.bfloat16
F32 = jnp.float32

L, HALF, SIDE, CH, GATES, TAPS = 128, 64, 16, 192, 768, 512
TWO, FOUR, EIGHT, FAR = 2, 4, 8, 18
PIECES = 6
PITCH = 24
IMG_ROWS = 26
STRIP = 24
MAIN = 288
EXT_M = 336
PLAIN_M = 256
INNER = 14
DIRS = ((-1, 0), (1, 0), (0, -1), (0, 1), (-1, -1), (-1, 1), (1, -1), (1, 1))
OPP = (1, 0, 3, 2, 7, 6, 5, 4)
STRIPS = ((1, 1, STRIP), (FAR, 1, STRIP), (2, 3, SIDE), (17, 3, SIDE))
STRIP_M = 80
EXT = (((1, FAR),), slice(0, 48))
PLAIN = (((2, SIDE),), None)
IN = (((3, INNER),), None)
EXT_OUT = (((1, 2), (17, 2)), slice(0, STRIP_M))
PLAIN_OUT = (((2, 1), (17, 1)), slice(48, STRIP_M))


def cell(er, ec):
    return er * PITCH + ec


def corner_src(d):
    return (TWO if DIRS[d][0] < 0 else SIDE), (TWO if DIRS[d][1] < 0 else SIDE)


def corner_dst(d):
    return (FAR if DIRS[d][0] < 0 else 0), (FAR if DIRS[d][1] < 0 else 0)


def near(e):
    return {TWO: TWO, SIDE: 17, FAR: FAR, 0: 1}[e]


def low_lanes(n):
    return lax.broadcasted_iota(jnp.int32, (n, L), 1) < HALF


def twice(v):
    return jnp.concatenate([v, v], axis=1)


def halves(v):
    lo, w = low_lanes(v.shape[0]), pltpu.roll(v, HALF, 1)
    return jnp.where(lo, v, w), jnp.where(lo, w, v)


def join(a, b):
    return jnp.where(low_lanes(a.shape[0]), a, b)


def flat(ref):
    return ref.reshape(ref.shape[0], TWO, IMG_ROWS * PITCH, L)


def put_col(img, er, ec, a, b):
    ref, x = img
    at = pl.ds(cell(er, ec), a.shape[0], stride=PITCH)
    flat(ref)[x, 0, at, :] = a
    flat(ref)[x, 1, at, :] = b


def get_col(img, lt, er, ec, n=SIDE):
    ref, x = img
    return flat(ref)[x, lt, pl.ds(cell(er, ec), n, stride=PITCH), :]


def put_rows(img, er, v):
    n = v.shape[0]
    v = v.reshape(n * SIDE, CH).astype(F32)
    put_body(img, er, v[:, :L], twice(v[:, L:]))


def put_body(img, er, a, b):
    n = a.shape[0] // SIDE
    ref, x = img
    for lt, v in enumerate((a, b)):
        ref[x, lt, pl.ds(er, n), TWO:FAR, :] = v.reshape(n, SIDE, L)


def pack_cols(dst, a0, b0, a1, b1):
    for i, v in enumerate((a0, a1, join(b0, b1))):
        dst[i] = v.astype(dst.dtype)


def unpack_cols(src):
    b0, b1 = halves(src[TWO].astype(F32))
    return src[0].astype(F32), b0, src[1].astype(F32), b1


def pack_corner(dst, img, d, a, b):
    er, ec = corner_src(d)
    ref, x = img
    for i in range(TWO):
        dst[TWO * i:TWO * i + TWO, :] = ref[x, 0, er + i, pl.ds(ec, TWO), :]
        dst[5 + i:6 + i, :] = join(ref[x, 1, er + i, pl.ds(ec, 1), :], ref[x, 1, er + i, pl.ds(ec + 1, 1), :])
    dst[FOUR:5, :] = a
    dst[7:EIGHT, :] = b


def unpack_corner(src, img, d):
    er, ec = corner_dst(d)
    ref, x = img
    for i in range(TWO):
        ref[x, 0, er + i, pl.ds(ec, TWO), :] = src[TWO * i:TWO * i + TWO, :]
        for j, v in enumerate(halves(src[5 + i:6 + i, :])):
            ref[x, 1, er + i, pl.ds(ec + j, 1), :] = v


def build_rows(img, lhs, first, n):
    tap, tail, _ = lhs
    ref, x = img
    rows = slice(first, first + n)
    lo = lax.broadcasted_iota(jnp.int32, (n, SIDE, L), TWO) < HALF
    for dc in range(3):
        tap[rows, :, dc * L:(dc + 1) * L] = ref[x, 0, rows, 1 + dc:17 + dc, :].astype(BF)
    b = [ref[x, 1, rows, 1 + dc:17 + dc, :] for dc in range(3)]
    tap[rows, :, 3 * L:] = jnp.where(lo, b[0], b[1]).astype(BF)
    m = n - TWO
    at = pl.ds(first * SIDE, m * SIDE)
    tail[at, :L] = jnp.where(lo[:m], b[TWO][:m], b[TWO][1:n - 1]).astype(BF).reshape(m * SIDE, L)
    tail[at, L:] = b[TWO][TWO:].astype(BF).reshape(m * SIDE, L)


def build_strips(img, lhs, which):
    _, tail, strip = lhs
    at = 0
    for ec, er, n in STRIPS:
        rows = slice(at, at + n)
        at += n
        if (ec, er, n) not in which:
            continue

        def col(lt, dr, dc):
            return get_col(img, lt, er - 1 + dr, ec - 1 + dc, n)

        for dr in range(3):
            for dc in range(3):
                strip[dr, rows, dc * L:(dc + 1) * L] = col(0, dr, dc).astype(BF)
            strip[dr, rows, 3 * L:] = join(col(1, dr, 0), col(1, dr, 1)).astype(BF)
        rows = slice(MAIN + rows.start, MAIN + rows.stop)
        tail[rows, :L] = join(col(1, 0, TWO), col(1, 1, TWO)).astype(BF)
        tail[rows, L:] = col(1, TWO, TWO).astype(BF)


def build(img, lhs, kind):
    if kind is EXT:
        build_rows(img, lhs, 0, 20)
        build_strips(img, lhs, STRIPS[:TWO])
    elif kind is PLAIN:
        build_rows(img, lhs, 1, FAR)
    elif kind is IN:
        build_rows(img, lhs, TWO, SIDE)
    elif kind is EXT_OUT:
        build_rows(img, lhs, 0, FOUR)
        build_rows(img, lhs, SIDE, FOUR)
        build_strips(img, lhs, STRIPS)
    else:
        build_rows(img, lhs, 1, 3)
        build_rows(img, lhs, SIDE, 3)
        build_strips(img, lhs, STRIPS[TWO:])


def operand(lhs, kind):
    tap, tail, strip = lhs
    runs, cut = kind
    blocks = []
    for dr in range(3):
        parts = [tap[er - 1 + dr:er - 1 + dr + n].reshape(n * SIDE, TAPS) for er, n in runs]
        blocks.append(parts + ([strip[dr, cut]] if cut else []))
    last = [tail[(er - 1) * SIDE:(er - 1 + n) * SIDE, :CH] for er, n in runs]
    if cut:
        last.append(tail[MAIN + cut.start:MAIN + cut.stop, :CH])
    return jnp.concatenate([jnp.concatenate(b, axis=0) for b in blocks + [last]], axis=1)


def conv(lhs, w, add, out, kind, first, parts):
    x = operand(lhs, kind)
    runs, cut = kind
    for p in parts:
        z = jnp.dot(x, w[:, TWO * p * L:TWO * (p + 1) * L], preferred_element_type=F32)
        for q in (TWO * p, TWO * p + 1):
            v = z[:, (q % TWO) * L:(q % TWO + 1) * L]

            def store(at, u):
                out[0][out[1], q, at, :] = u + (add[0][add[1], q, at, :] if isinstance(add, tuple) else add[q:q + 1, :])

            m = 0
            for er, n in runs:
                store(pl.ds((er - first) * SIDE, n * SIDE), v[m:m + n * SIDE])
                m += n * SIDE
            if cut and not cut.start:
                store(pl.ds(MAIN, TWO * STRIP), v[m:m + TWO * STRIP])
                m += TWO * STRIP
            if kind is EXT_OUT or kind is PLAIN_OUT:
                for side in range(TWO):
                    store(pl.ds((3 - first) * SIDE + 15 * side, INNER, stride=SIDE), v[m:m + INNER])
                    m += SIDE


def gates(z, c0, c1):
    lo = low_lanes(c0.shape[0])
    half = jnp.where(lo, 0.5, 1.0).astype(F32)
    off = jnp.where(lo, 0.5, 0.0).astype(F32)

    def sigmoid(v):
        return 0.5 * jnp.tanh(0.5 * v) + 0.5

    in0, a1, a2, out0 = [sigmoid(v) for v in z[:FOUR]]
    a4 = half * jnp.tanh(half * z[FOUR]) + off
    a5 = jnp.tanh(z[5])
    forget0 = pltpu.roll(jnp.where(lo, a2, a1), HALF, 1)
    cand0 = pltpu.roll(jnp.where(lo, a5, a4), HALF, 1)
    in_forget1 = jnp.where(lo, a1, a2)
    out_cand1 = jnp.where(lo, a4, a5)
    c0n = forget0 * c0 + in0 * cand0
    prod = in_forget1 * jnp.where(lo, pltpu.roll(out_cand1, HALF, 1), c1)
    c1n = prod + pltpu.roll(prod, HALF, 1)
    h0 = out0 * jnp.tanh(c0n)
    h1, _ = halves(out_cand1 * jnp.tanh(c1n))
    return h0.astype(BF), h1.astype(BF), c0n, c1n


def kernel(frames, w_x, w_h, bias_in, h_init, c_init, h_all, c_final,
           fr, hin, cin, bias_v, bias, wx, wh, imgx, imgh, cst, tapx, tailx, stripx, tapy, taily, stripy, taph, tailh, striph, tapi, taili,
           gext, gpl, zext, zpl,
           s_xcol, s_xdiag, r_xrow, r_xcol, r_xdiag,
           s_hcol, s_ccol, s_diag, r_hrow, r_hcol, r_crow, r_ccol, r_diag,
           lsem, wsem, xs_sem, xr_sem, e_s, e_r, *, shape):
    lhs_x, lhs_y, lhs_h, lhs_i = (tapx, tailx, stripx), (tapy, taily, stripy), (taph, tailh, striph), (tapi, taili, None)
    n_rows, n_cols = shape
    row, col = lax.axis_index("rows"), lax.axis_index("cols")
    grp = lax.axis_index("batch")

    def has(d):
        dr, dc = DIRS[d]
        rr, cc = row + dr, col + dc
        return (rr >= 0) & (rr < n_rows) & (cc >= 0) & (cc < n_cols)

    def peer(d):
        return (grp, col + DIRS[d][1], row + DIRS[d][0])

    have = [has(d) for d in range(EIGHT)]

    def each(f, dirs=(TWO, 3, FOUR, 5, 6, 7, 0, 1)):
        for d in dirs:
            @pl.when(have[d])
            def _(d=d):
                f(d)

    def start(copies):
        for cp in copies:
            cp.start()

    def exchanged(copies, d):
        for cp in copies(OPP[d]):
            cp.wait_recv()
        for cp in copies(d):
            cp.wait_send()

    load_h = pltpu.make_async_copy(h_init, hin, lsem.at[0])
    load_c = pltpu.make_async_copy(c_init, cin, lsem.at[1])
    load_b = pltpu.make_async_copy(bias_in, bias_v, lsem.at[TWO])
    load_f = [pltpu.make_async_copy(frames.at[pl.ds(TWO * k, TWO)], fr.at[pl.ds(TWO * k, TWO)], lsem.at[3 + k]) for k in range(FOUR)]
    load_w = [[], []]
    for i, (src, dst) in enumerate(((w_x, wx), (w_h, wh))):
        for dr in range(3):
            for dc in range(3):
                at = dr * TAPS + 3 * L + dc * HALF if dc < TWO else 3 * TAPS + dr * HALF
                for c_at, n, k_at in ((0, L, dr * TAPS + dc * L), (L, HALF, at)):
                    load_w[i].append(pltpu.make_async_copy(src.at[dr, dc, pl.ds(c_at, n)], dst.at[pl.ds(k_at, n)], wsem.at[i, len(load_w[i])]))
    start([load_f[0], load_h, load_c, load_b] + load_w[0])

    barrier = pltpu.get_barrier_semaphore()
    each(lambda d: pl.semaphore_signal(barrier, inc=1, device_id=peer(d), device_id_type=MESH))

    def blank(d):
        refs = (r_xrow, r_hrow, r_crow) if d < TWO else (r_xcol, r_hcol, r_ccol) if d < FOUR else (r_xdiag, r_diag)
        for ref in refs:
            ref[:, d % FOUR if d > 3 else d % TWO] = jnp.zeros((ref.shape[0],) + ref.shape[TWO:], ref.dtype)

    def frame_stage(k):
        for odd in range(TWO):
            for s in range(TWO):
                put_rows((imgx, FOUR * k + TWO * odd + s), TWO, fr[TWO * k + odd, s])
        for side in range(TWO):
            ec = (TWO + 15 * side, 3 + 13 * side)
            for s in range(TWO):
                img = (imgx, FOUR * k + s)
                pack_cols(s_xcol.at[TWO * k, side, s], *[get_col(img, lt, TWO, e) for e in ec for lt in range(TWO)])
            pack_cols(s_xcol.at[TWO * k + 1, side, 0], *[get_col((imgx, FOUR * k + TWO + s), lt, TWO, ec[0]) for s in range(TWO) for lt in range(TWO)])
        for d in range(FOUR, EIGHT):
            er, ec = [near(e) for e in corner_src(d)]
            for s in range(TWO):
                pack_corner(s_xdiag.at[k, d - FOUR, s], (imgx, FOUR * k + s), d, *[imgx[FOUR * k + TWO + s, lt, er, pl.ds(ec, 1), :] for lt in range(TWO)])

    def frame_copies(k, odd, d):
        f = TWO * k + odd

        def mk(src, dst):
            return [pltpu.make_async_remote_copy(src_ref=src, dst_ref=dst, send_sem=xs_sem.at[f, d], recv_sem=xr_sem.at[f, d], device_id=peer(d), device_id_type=MESH)]

        n = 1 if odd else TWO
        if d < TWO:
            at = SIDE - n if d else 0
            return mk(fr.at[f, :, pl.ds(at, n)], r_xrow.at[f, d, :, pl.ds(d if odd else 0, n)])
        if d < FOUR:
            return mk(s_xcol.at[f, d - TWO, pl.ds(0, n)], r_xcol.at[f, d - TWO, pl.ds(0, n)])
        return [] if odd else mk(s_xdiag.at[k, d - FOUR], r_xdiag.at[k, d - FOUR])

    def both_frames(k):
        return lambda d: frame_copies(k, 0, d) + frame_copies(k, 1, d)

    def frame_wait(k):
        each(lambda d: exchanged(both_frames(k), d))

    def frame_fill(k, odd, s):
        f = TWO * k + odd
        img = (imgx, TWO * f + s)
        for d in range(TWO):
            i, n = (d, 1) if odd else (0, TWO)
            put_rows(img, i + FAR * (1 - d), r_xrow[f, d, s, pl.ds(i, n)])
            ec = (1, 0) if d else (FAR, FAR + 1)
            if odd:
                b = halves(r_xcol[f, d, 0, TWO].astype(F32))
                b = b[s] if isinstance(s, int) else jnp.where(flag(s == 0, SIDE), *b)
                put_col(img, TWO, ec[0], r_xcol[f, d, 0, s].astype(F32), b)
            else:
                ab = unpack_cols(r_xcol[f, d, s])
                put_col(img, TWO, ec[0], *ab[:TWO])
                put_col(img, TWO, ec[1], *ab[TWO:])
        for d in range(FOUR, EIGHT):
            src = r_xdiag.at[k, d - FOUR, s]
            if odd:
                er, ec = [near(e) for e in corner_dst(d)]
                imgx[TWO * f + s, 0, er, pl.ds(ec, 1), :] = src[FOUR:5, :]
                imgx[TWO * f + s, 1, er, pl.ds(ec, 1), :] = src[7:EIGHT, :]
            else:
                unpack_corner(src, img, d)

    def x_build(k, odd, s, kind):
        build((imgx, FOUR * k + TWO * odd + s), lhs_y if odd else lhs_x, kind)

    def x_conv(s, odd, kind, parts=range(3)):
        conv(lhs_y if odd else lhs_x, wx, bias, (gpl if odd else gext, s), kind, 1 + odd, parts)

    def state_copies(e, s, d, hsrc):
        x = TWO * e + s
        if d < TWO:
            refs = ((hsrc.at[pl.ds(INNER * d, TWO)], r_hrow.at[x, d]), (cst.at[s, :, pl.ds(SIDE + 240 * d, SIDE)], r_crow.at[x, d]))
        elif d < FOUR:
            refs = ((s_hcol.at[s, d - TWO], r_hcol.at[x, d - TWO]), (s_ccol.at[s, d - TWO], r_ccol.at[x, d - TWO]))
        else:
            refs = ((s_diag.at[s, d - FOUR], r_diag.at[x, d - FOUR]),)
        return [pltpu.make_async_remote_copy(src_ref=refs[i][0], dst_ref=refs[i][1], send_sem=e_s.at[x, d + EIGHT * i], recv_sem=e_r.at[x, d + EIGHT * i], device_id=peer(d), device_id_type=MESH) for i in range(len(refs))]

    def state_stage(s):
        img = (imgh, s)
        for side in range(TWO):
            ec = (TWO + 15 * side, 3 + 13 * side)
            pack_cols(s_hcol.at[s, side], *[get_col(img, lt, TWO, e) for e in ec for lt in range(TWO)])
            c0, c1 = [cst[s, lt, pl.ds(SIDE + 15 * side, SIDE, stride=SIDE), :] for lt in range(TWO)]
            s_ccol[s, side, :SIDE] = c0
            s_ccol[s, side, SIDE:] = join(c1[:EIGHT], c1[EIGHT:])
        for d in range(FOUR, EIGHT):
            er, ec = [near(e) for e in corner_src(d)]
            at = pl.ds((er - 1) * SIDE + ec - TWO, 1)
            pack_corner(s_diag.at[s, d - FOUR], img, d, cst[s, 0, at, :], cst[s, 1, at, :])

    def state_send(e, s, hsrc):
        each(lambda d: start(state_copies(e, s, d, hsrc)))

    def state_wait(e, s):
        each(lambda d: exchanged(lambda d: state_copies(e, s, d, hin.at[s]), d))

    def state_fill(e, s):
        img = (imgh, s)
        x = TWO * e + s
        for d in range(TWO):
            put_rows(img, FAR * (1 - d), r_hrow[x, d])
            cst[s, :, pl.ds(272 * (1 - d), SIDE), :] = r_crow[x, d]
            ab = unpack_cols(r_hcol[x, d])
            ec = (1, 0) if d else (FAR, FAR + 1)
            put_col(img, TWO, ec[0], *ab[:TWO])
            put_col(img, TWO, ec[1], *ab[TWO:])
            v = r_ccol[x, d]
            m = MAIN + STRIP * (1 - d) + 1
            cst[s, 0, pl.ds(m, SIDE), :] = v[:SIDE]
            cst[s, 1, pl.ds(m, SIDE), :] = jnp.concatenate(halves(v[SIDE:]), axis=0)
        for d in range(FOUR, EIGHT):
            src = r_diag.at[x, d - FOUR]
            unpack_corner(src, img, d)
            er, ec = corner_dst(d)
            m = MAIN + (STRIP if ec else 0) + (17 if er else 0)
            cst[s, 0, pl.ds(m, 1), :] = src[FOUR:5, :]
            cst[s, 1, pl.ds(m, 1), :] = src[7:EIGHT, :]

    def at_side(d):
        return have[d]

    def flag(cond, n):
        return jnp.full((n, L), jnp.where(cond, 1, 0).astype(jnp.int32)) > 0

    def update(s, t, ext, last=False):
        img = (imgh, s)
        z_ref = zext if ext else zpl

        def one(m, n):
            zm = m if ext else m - SIDE
            z = [z_ref[s, p, zm:zm + n, :] for p in range(PIECES)]
            h0, h1, c0, c1 = gates(z, cst[s, 0, m:m + n, :], cst[s, 1, m:m + n, :])
            cst[s, 0, m:m + n, :] = c0
            cst[s, 1, m:m + n, :] = c1
            return h0, h1, c0, c1

        er, end = (1, FAR + 1) if ext else (TWO, FAR)
        while er < end:
            n = 1 if er == 1 or er == end - 1 else TWO
            h0, h1, c0, c1 = one((er - 1) * SIDE, n * SIDE)
            if 1 < er < FAR:
                at = pl.ds(er - TWO, n)
                h_all[t, s, at, :, :L] = h0.reshape(n, SIDE, L)
                h_all[t, s, at, :, L:] = h1[:, :HALF].reshape(n, SIDE, HALF)
            if last:
                c_final[s, at, :, :L] = c0.reshape(n, SIDE, L)
                c_final[s, at, :, L:] = c1[:, :HALF].reshape(n, SIDE, HALF)
            else:
                f0, f1 = h0.astype(F32), h1.astype(F32)
                if er == 1 or er == FAR:
                    ok = flag(at_side(er // FAR), n * SIDE)
                    f0, f1 = jnp.where(ok, f0, 0.0), jnp.where(ok, f1, 0.0)
                put_body(img, er, f0, f1)
            er += n
        if not ext:
            return
        pos = lax.broadcasted_iota(jnp.int32, (STRIP, L), 0)
        for side in range(TWO):
            ok = flag(at_side(TWO + side), STRIP) & (flag(at_side(0), STRIP) | (pos > 0)) & (flag(at_side(1), STRIP) | (pos < 17))
            h0, h1, _, _ = one(MAIN + STRIP * side, STRIP)
            put_col(img, 1, 1 + 17 * side, jnp.where(ok, h0.astype(F32), 0.0), jnp.where(ok, h1.astype(F32), 0.0))

    def h_build(s, kind):
        build((imgh, s), lhs_i if kind is IN else lhs_h, kind)

    def h_conv(s, kind):
        if kind is PLAIN:
            conv(lhs_h, wh, (gpl, s), (zpl, s), kind, TWO, range(3))
        else:
            conv(lhs_i if kind is IN else lhs_h, wh, (gext, s), (zext, s), kind, 1, range(3))

    load_f[0].wait()
    frame_stage(0)
    load_h.wait()
    load_c.wait()
    def first_state(s, _):
        put_rows((imgh, s), TWO, hin[s])
        v = cin[s].reshape(PLAIN_M, CH)
        at = pl.ds(SIDE, PLAIN_M)
        cst[s, 0, at, :] = v[:, :L]
        cst[s, 1, at, :] = twice(v[:, L:])
        state_stage(s)
        return 0

    lax.fori_loop(0, TWO, first_state, 0)
    near_rows = 1 + have[0].astype(jnp.int32) + have[1].astype(jnp.int32)
    near_cols = 1 + have[TWO].astype(jnp.int32) + have[3].astype(jnp.int32)
    pl.semaphore_wait(barrier, near_rows * near_cols - 1)
    each(lambda d: start(frame_copies(0, 0, d) + state_copies(0, 0, d, hin.at[0]) + frame_copies(0, 1, d) + state_copies(0, 1, d, hin.at[1])))
    start(load_w[1] + load_f[1:])
    for d in range(EIGHT):
        @pl.when(jnp.logical_not(have[OPP[d]]))
        def _(d=d):
            blank(d)
    load_b.wait()
    for p in range(PIECES):
        bias[p:p + 1, :] = bias_v[pl.ds(p * L, L)].reshape(1, L)
    for cp in load_w[0]:
        cp.wait()
    for s in range(TWO):
        for odd in range(TWO - s):
            x_build(0, odd, s, IN)
            x_conv(s, odd, IN)
    for cp in load_w[1] + load_f[1:]:
        cp.wait()

    def stage_body(k, _):
        frame_stage(k)
        each(lambda d: start(both_frames(k)(d)))
        return 0

    lax.fori_loop(1, FOUR, stage_body, 0)
    h_build(0, IN)
    h_conv(0, IN)
    frame_wait(0)
    for s in range(TWO):
        for odd in range(TWO):
            kind = (PLAIN if s else PLAIN_OUT) if odd else EXT_OUT
            frame_fill(0, odd, s)
            x_build(0, odd, s, kind)
            x_conv(s, odd, kind, (0,) if kind is PLAIN else range(3))

    def left_over(s):
        x_conv(s, 1, PLAIN, (1, TWO))
        h_build(s, IN)
        h_conv(s, IN)

    def round_body(k, _):
        frame_wait(k + 1)
        for s in range(TWO):
            state_wait(k, s)
            left_over(1 - s)
            state_fill(k, s)
            h_build(s, EXT_OUT)
            h_conv(s, EXT_OUT)
            frame_fill(k + 1, 0, s)
            x_build(k + 1, 0, s, EXT)
            x_conv(s, 0, EXT, (0, 1))
            update(s, TWO * k, True)
            h_build(s, PLAIN)
            h_conv(s, PLAIN)
            frame_fill(k + 1, 1, s)
            x_build(k + 1, 1, s, PLAIN)
            x_conv(s, 0, EXT, (TWO,))
            x_conv(s, 1, PLAIN, (0,))
            update(s, TWO * k + 1, False)
            state_stage(s)
            state_send(k + 1, s, h_all.at[TWO * k + 1, s])
        return 0

    lax.fori_loop(0, 3, round_body, 0)
    last = 3
    for s in range(TWO):
        state_wait(last, s)
        if s == 0:
            left_over(1)
        state_fill(last, s)
        h_build(s, EXT_OUT)
        h_conv(s, EXT_OUT)
    update(0, TWO * last, True)
    h_build(0, PLAIN)
    h_conv(0, PLAIN)
    update(1, TWO * last, True)
    h_build(1, PLAIN)
    update(0, TWO * last + 1, False, True)
    h_conv(1, PLAIN)
    update(1, TWO * last + 1, False, True)


def solution(mesh):
    shape = (mesh.shape["rows"], mesh.shape["cols"])
    frame_spec = P(None, "batch", "rows", "cols", None)
    state_spec = P("batch", "rows", "cols", None)
    any_spec = pl.BlockSpec(memory_space=pl.ANY)
    vmem = pl.BlockSpec(memory_space=pltpu.VMEM)

    def local_run(frames, w_x, w_h, gate_bias, h_init, c_init):
        V = pltpu.VMEM
        D = pltpu.SemaphoreType.DMA
        lhs = [V((20, SIDE, TAPS), BF), V((MAIN + STRIP_M, TWO * L), BF), V((3, STRIP_M, TAPS), BF)]
        pair = (TWO, TWO)
        scratch = [
            V(frames.shape, BF), V(h_init.shape, BF), V(c_init.shape, F32), V(gate_bias.shape, F32), V((EIGHT, L), F32),
            V((9 * CH, GATES), BF), V((9 * CH, GATES), BF),
            V((SIDE, TWO, IMG_ROWS, PITCH, L), F32), V(pair + (IMG_ROWS, PITCH, L), F32), V(pair + (EXT_M, L), F32),
            *lhs, *lhs, *lhs, *lhs[:TWO],
            V((TWO, PIECES, EXT_M, L), F32), V((TWO, PIECES, PLAIN_M, L), F32), V((TWO, PIECES, EXT_M, L), F32), V((TWO, PIECES, PLAIN_M, L), F32),
            V((EIGHT, TWO, TWO, 3, SIDE, L), BF), V((FOUR, FOUR, TWO, EIGHT, L), F32),
            V((EIGHT, TWO, TWO, TWO, SIDE, CH), BF), V((EIGHT, TWO, TWO, 3, SIDE, L), BF), V((FOUR, FOUR, TWO, EIGHT, L), F32),
            V(pair + (3, SIDE, L), BF), V(pair + (STRIP, L), F32), V((TWO, FOUR, EIGHT, L), F32),
            V((EIGHT, TWO, TWO, SIDE, CH), BF), V((EIGHT, TWO, 3, SIDE, L), BF), V((EIGHT, TWO, TWO, SIDE, L), F32), V((EIGHT, TWO, STRIP, L), F32), V((EIGHT, FOUR, EIGHT, L), F32),
            D((7,)), D((TWO, FAR)), D((EIGHT, EIGHT)), D((EIGHT, EIGHT)), D((EIGHT, 12)), D((EIGHT, 12)),
        ]
        return pl.pallas_call(
            functools.partial(kernel, shape=shape),
            out_shape=[V(frames.shape, BF), V(c_init.shape, F32)],
            in_specs=[any_spec] * 6,
            out_specs=[vmem, vmem],
            scratch_shapes=scratch,
            compiler_params=pltpu.CompilerParams(collective_id=0, has_side_effects=True, vmem_limit_bytes=60 * 1024 * 1024),
            name="convlstm",
        )(frames, w_x, w_h, gate_bias, h_init, c_init)

    return jax.shard_map(local_run, mesh=mesh, in_specs=(frame_spec, P(), P(), P(), state_spec, state_spec), out_specs=(frame_spec, state_spec), check_vma=False)
```
